32 devices in a mesh: dp: 4 (over y, z), ep: 8 (over x, core).
Axes of the slice: x: 4, y: 2, z: 2, core: 2. Of those that a mesh axis runs over, the one named last changes fastest.
The devices are a block of a 4x4x8 slice.
Arguments:
- hidden: bfloat16 [8192, 2048], P(('dp', 'ep')), parts along dimension 0
- router_w: float32 [2048, 32], replicated
- expert_ids: int32 [8192, 2], P(('dp', 'ep')), parts along dimension 0
- w_gate: bfloat16 [32, 2048, 3072], P('ep')
- w_up: bfloat16 [32, 2048, 3072], P('ep')
- w_down: bfloat16 [32, 3072, 2048], P('ep')
- post_scale: float32 [2], replicated
Outputs:
- output: bfloat16 [8192, 2048], P(('dp', 'ep')), parts along dimension 0
There are 4 independent parts. The reference program is written for one: setup_inputs(seed, part) draws one part's arguments, and reference() takes and returns one part's arrays. A program takes and returns all parts, laid end to end along the dimension named above; an argument that names none is the same for every part.
All inputs are finite; a program needn't handle non-finite values.
Results may differ from the reference program's by a relative error of at most 0.001.
Values are sent between devices in bfloat16 or wider.
A program may use at most 768 MiB of HBM per device.

```python
import jax
import jax.numpy as jnp
from jax import lax

GROUP_SIZE = 8
TOKENS_DEV = 256
EXPERTS = 32
HIDDEN = 2048
FFN_DIM = 3072
TOP_K = 2
BATCH_ROWS = GROUP_SIZE * TOKENS_DEV
HOT_COUNT = max(1, EXPERTS // 8)
CAPACITY = TOKENS_DEV // HOT_COUNT
MAX_ROWS = GROUP_SIZE * CAPACITY


def draw_routing(ids_key, part):
    order_key, shard_key = jax.random.split(ids_key)
    expert_order = jax.random.permutation(order_key, EXPERTS)
    hot_ids = expert_order[:HOT_COUNT]
    cold_ids = expert_order[HOT_COUNT:]
    shard_keys = jax.random.split(jax.random.fold_in(shard_key, part), GROUP_SIZE)

    def one_shard(one_key):
        tok_key, cold_key, swap_key = jax.random.split(one_key, 3)
        tok_rank = jax.random.permutation(tok_key, TOKENS_DEV)
        cold_mix = jax.random.permutation(cold_key, cold_ids)
        first_pick = hot_ids[tok_rank % HOT_COUNT]
        second_pick = cold_mix[tok_rank % (EXPERTS - HOT_COUNT)]
        swapped = jax.random.randint(swap_key, (TOKENS_DEV,), 0, 2) == 1
        return jnp.stack([jnp.where(swapped, second_pick, first_pick), jnp.where(swapped, first_pick, second_pick)], axis=1)

    return jax.vmap(one_shard)(shard_keys).reshape(BATCH_ROWS, TOP_K).astype(jnp.int32)


def draw_experts(weight_key, row_count, col_count):
    expert_keys = jax.random.split(weight_key, EXPERTS)
    return lax.map(lambda one_key: (jax.random.normal(one_key, (row_count, col_count), jnp.float32) * row_count ** -0.5).astype(jnp.bfloat16), expert_keys)


def setup_inputs(seed: int = 0, part: int = 0) -> dict:
    base_key = jax.random.key(seed)
    hid_key, route_key, gate_key, up_key, down_key, post_key, ids_key = jax.random.split(base_key, 7)
    hidden = jax.random.normal(jax.random.fold_in(hid_key, part), (BATCH_ROWS, HIDDEN), jnp.float32).astype(jnp.bfloat16)
    router_w = jax.random.normal(route_key, (HIDDEN, EXPERTS), jnp.float32) * (0.4 * HIDDEN ** -0.5)
    w_gate = draw_experts(gate_key, HIDDEN, FFN_DIM)
    w_up = draw_experts(up_key, HIDDEN, FFN_DIM)
    w_down = draw_experts(down_key, FFN_DIM, HIDDEN)
    post_scale = jax.random.uniform(post_key, (2,), jnp.float32, jnp.array([0.5, 1.0], jnp.float32), jnp.array([1.0, 2.0], jnp.float32))
    expert_ids = draw_routing(ids_key, part)
    return {'hidden': hidden, 'router_w': router_w, 'expert_ids': expert_ids, 'w_gate': w_gate, 'w_up': w_up, 'w_down': w_down, 'post_scale': post_scale}


def reference(hidden, router_w, expert_ids, w_gate, w_up, w_down, post_scale):
    hid_wide = hidden.astype(jnp.float32)
    logits = jnp.dot(hid_wide, router_w, preferred_element_type=jnp.float32)
    router_prob = jax.nn.softmax(logits, axis=-1)
    picked = jnp.take_along_axis(router_prob, expert_ids, axis=1)
    gates = picked / jnp.sum(picked, axis=1, keepdims=True)

    def add_expert(running_sum, expert):
        hit_mask = expert_ids == expert
        tok_gate = jnp.sum(jnp.where(hit_mask, gates, 0.0), axis=1)
        chosen = jnp.any(hit_mask, axis=1)
        row_index = jnp.nonzero(chosen, size=MAX_ROWS, fill_value=0)[0]
        in_range = jnp.arange(MAX_ROWS) < jnp.sum(chosen)
        tok_rows = hidden[row_index]
        gate_in = jnp.dot(tok_rows, w_gate[expert], preferred_element_type=jnp.float32)
        up_in = jnp.dot(tok_rows, w_up[expert], preferred_element_type=jnp.float32)
        middle = (jax.nn.silu(gate_in) * up_in).astype(jnp.bfloat16)
        expert_out = jnp.dot(middle, w_down[expert], preferred_element_type=jnp.float32).astype(jnp.bfloat16)
        row_weight = jnp.where(in_range, tok_gate[row_index], 0.0)
        running_sum = running_sum.at[row_index].add(row_weight[:, None] * expert_out.astype(jnp.float32))
        return running_sum, None

    mixed, _ = lax.scan(add_expert, jnp.zeros((BATCH_ROWS, HIDDEN), jnp.float32), jnp.arange(EXPERTS))
    return (post_scale[0] * hid_wide + post_scale[1] * mixed).astype(jnp.bfloat16)
```

```python
import functools

import jax
import jax.numpy as jnp
from jax import lax
from jax.experimental import pallas as pl
from jax.experimental.pallas import tpu as pltpu
from jax.sharding import PartitionSpec as P

MESH = pl.DeviceIdType.MESH
PIECES = 4
TILE = 128
GRAN = 16
F32 = jnp.float32
BF16 = jnp.bfloat16


def dispatch_kernel(n, le, cap, h_ref, wrt_ref, idst_ref, xs_ref, qmap_ref, meta_ref, comb_ref,
                    all_h, all_ids, x_buf, send_sem, ring_sem, pair_sem, x_sem, ids_send, ids_recv):
    ep = lax.axis_index("ep")
    chips = n // 2
    x, c = ep // 2, ep % 2

    def dev(xx, cc):
        return lax.rem(xx + 2 * chips, chips) * 2 + cc

    xp, xm, pa = dev(x + 1, c), dev(x - 1, c), dev(x, 1 - c)
    bar = pltpu.get_barrier_semaphore()
    for o in range(1, n):
        pl.semaphore_signal(bar, inc=1, device_id={"ep": lax.rem(ep + o, n)}, device_id_type=MESH)
    pl.semaphore_wait(bar, n - 1)

    tokens, _ = h_ref.shape
    rows = tokens // PIECES
    started = []

    for o in range(1, n):
        cp = pltpu.make_async_remote_copy(
            src_ref=idst_ref, dst_ref=all_ids.at[ep], send_sem=ids_send.at[o], recv_sem=ids_recv.at[o],
            device_id={"ep": lax.rem(ep + o, n)}, device_id_type=MESH)
        cp.start()
        started.append(cp)
    own_ids = pltpu.make_async_copy(idst_ref, all_ids.at[ep], ids_recv.at[0])
    own_ids.start()

    count = [0]

    def push(src, blk, p, to, rsem):
        cp = pltpu.make_async_remote_copy(
            src_ref=src, dst_ref=all_h.at[blk, pl.ds(p * rows, rows)], send_sem=send_sem.at[count[0]], recv_sem=rsem,
            device_id={"ep": to}, device_id_type=MESH)
        count[0] += 1
        cp.start()
        started.append(cp)

    def arrive(blk, p, sem):
        ref = all_h.at[blk, pl.ds(p * rows, rows)]
        pltpu.make_async_remote_copy(src_ref=ref, dst_ref=ref, send_sem=send_sem.at[0], recv_sem=sem,
                                     device_id={"ep": pa}, device_id_type=MESH).wait_recv()

    last = PIECES - 1
    for s in range(PIECES):
        push(h_ref.at[pl.ds(s * rows, rows)], ep, s, xp, ring_sem.at[0, s])
        push(h_ref.at[pl.ds((last - s) * rows, rows)], ep, last - s, xm, ring_sem.at[1, last - s])
    for s in range(PIECES):
        push(h_ref.at[pl.ds(s * rows, rows)], ep, s, pa, pair_sem.at[0, s])

    own_ids.wait()
    for o in range(1, n):
        ref = all_ids.at[lax.rem(ep + n - o, n)]
        pltpu.make_async_remote_copy(src_ref=ref, dst_ref=ref, send_sem=ids_send.at[o], recv_sem=ids_recv.at[o],
                                     device_id={"ep": pa}, device_id_type=MESH).wait_recv()
    ids0 = all_ids[:, 0, :]
    ids1 = all_ids[:, 1, :]
    experts = n * le
    upper = (lax.broadcasted_iota(jnp.int32, (tokens, tokens), 0)
             < lax.broadcasted_iota(jnp.int32, (tokens, tokens), 1)).astype(F32).astype(BF16)

    def hits(lo, hi):
        return (jnp.where((ids0 >= lo) & (ids0 < hi), 1.0, 0.0) + jnp.where((ids1 >= lo) & (ids1 < hi), 1.0, 0.0))

    lane = lax.broadcasted_iota(jnp.int32, (n, le * cap), 1)
    lane_m = lax.broadcasted_iota(jnp.int32, meta_ref.shape, 1)
    qmap = jnp.full((n, le * cap), -1.0, F32)
    meta = jnp.zeros(meta_ref.shape, F32)
    offset = jnp.where(c > 0, 1.0, 0.0) * jnp.sum(hits(x * 2 * le, x * 2 * le + le), axis=1, keepdims=True)
    slots = []
    for l in range(le):
        e = ep * le + l
        mask = jnp.where((ids0 == e) | (ids1 == e), 1.0, 0.0)
        rank = jnp.dot(mask.astype(BF16), upper, preferred_element_type=F32)
        slots.append(jnp.where(mask > 0.5, rank, -1.0).astype(jnp.int32))
        cnt = jnp.sum(mask, axis=1, keepdims=True)
        inside = lane - l * cap
        insidef = inside.astype(F32)
        qmap = jnp.where((inside >= 0) & (inside < cap) & (insidef < cnt), offset + insidef, qmap)
        meta = jnp.where(lane_m == l, cnt, meta)
        offset = offset + cnt
    qmap_ref[...] = qmap.astype(jnp.int32)
    worst = jnp.zeros((n, 1), F32)
    for j in range(chips):
        worst = jnp.maximum(worst, jnp.sum(hits(j * 2 * le, (j + 1) * 2 * le), axis=1, keepdims=True))
    worst = jnp.max(worst, axis=0, keepdims=True)
    meta_ref[...] = jnp.where(lane_m == le, worst, meta).astype(jnp.int32)

    own0, own1 = idst_ref[0:1, :], idst_ref[1:2, :]
    sub = lax.broadcasted_iota(jnp.int32, (experts, tokens), 0)
    logits = lax.dot_general(wrt_ref[...], h_ref[...].astype(F32), (((1,), (1,)), ((), ())),
                             precision=lax.Precision.HIGHEST, preferred_element_type=F32)
    ex = jnp.exp(logits - jnp.max(logits, axis=0, keepdims=True))
    prob = ex / jnp.sum(ex, axis=0, keepdims=True)
    pick0, pick1 = sub == own0, sub == own1
    p0 = jnp.sum(jnp.where(pick0, prob, 0.0), axis=0, keepdims=True)
    p1 = jnp.sum(jnp.where(pick1, prob, 0.0), axis=0, keepdims=True)
    hot = jnp.where(pick0 | pick1, 1.0, 0.0)
    rank = jnp.dot(hot.astype(BF16), upper, preferred_element_type=F32)
    ei = lax.broadcasted_iota(jnp.int32, (experts, experts), 0)
    ej = lax.broadcasted_iota(jnp.int32, (experts, experts), 1)
    before = ((ei // (2 * le) == ej // (2 * le)) & (ej < ei)).astype(F32).astype(BF16)
    total = jnp.broadcast_to(jnp.sum(hot, axis=1, keepdims=True), (experts, 128)).astype(BF16)
    base = jnp.dot(before, total, preferred_element_type=F32)[:, 0:1]
    where = rank + base
    pos0 = jnp.sum(jnp.where(pick0, where, 0.0), axis=0, keepdims=True)
    pos1 = jnp.sum(jnp.where(pick1, where, 0.0), axis=0, keepdims=True)
    chip0, chip1 = (own0 // (2 * le)).astype(F32), (own1 // (2 * le)).astype(F32)
    row = lax.broadcasted_iota(jnp.int32, (128, tokens), 0)
    packed = jnp.zeros((128, tokens), F32)
    for k, v in enumerate((pos0, pos1, p0 / (p0 + p1), p1 / (p0 + p1), chip0, chip1)):
        packed = jnp.where(row == k, v, packed)
    comb_ref[...] = packed.T

    slot_row = lax.broadcasted_iota(jnp.int32, (cap, tokens), 0)
    moves = []

    def place(i, k):
        all_slots = []
        for l in range(le):
            one = slots[l]
            pick = jnp.sum(jnp.where(lax.broadcasted_iota(jnp.int32, one.shape, 0) == i, one, 0), axis=0, keepdims=True)
            all_slots.append((pick == slot_row).astype(F32).astype(BF16))
        rows_hot = jnp.concatenate(all_slots, axis=0)
        src = h_ref if k == 0 else all_h.at[i]
        half = x_buf.shape[2] // 2
        for q in range(2):
            cols = pl.ds(q * half, half)
            x_buf[k % 2, :, cols] = jnp.dot(rows_hot, src[:, cols], preferred_element_type=F32).astype(BF16)
        for l in range(le):
            cp = pltpu.make_async_copy(x_buf.at[k % 2, pl.ds(l * cap, cap)], xs_ref.at[l, i], x_sem.at[k, l])
            cp.start()
            moves.append(cp)

    def drain(k):
        for cp in moves[k * le:(k + 1) * le]:
            cp.wait()

    place(ep, 0)

    bm, bp, b2 = dev(x - 1, c), dev(x + 1, c), dev(x + 2, c)
    for s in range(PIECES):
        q = last - s
        arrive(bm, s, ring_sem.at[0, s])
        ref = all_h.at[bm, pl.ds(s * rows, rows)]
        if s < PIECES // 2:
            push(ref, bm, s, xp, ring_sem.at[2, s])
        push(ref, bm, s, pa, pair_sem.at[1, s])
        arrive(bp, q, ring_sem.at[1, q])
        ref = all_h.at[bp, pl.ds(q * rows, rows)]
        if s < PIECES // 2:
            push(ref, bp, q, xm, ring_sem.at[2, q])
        push(ref, bp, q, pa, pair_sem.at[2, q])
    for s in range(PIECES // 2):
        for q in (s, last - s):
            arrive(b2, q, ring_sem.at[2, q])
            push(all_h.at[b2, pl.ds(q * rows, rows)], b2, q, pa, pair_sem.at[3, q])
    def landed(i, xx):
        for s in range(PIECES):
            arrive(dev(xx, 1 - c), s, pair_sem.at[i, s])

    landed(0, x)
    place(pa, 1)
    for k, blk in enumerate((bm, bp)):
        drain(k)
        place(blk, 2 + k)
    for k, xx in enumerate((x - 1, x + 1)):
        landed(1 + k, xx)
        drain(2 + k)
        place(dev(xx, 1 - c), 4 + k)
    drain(4)
    place(b2, 6)
    landed(3, x + 2)
    drain(5)
    place(dev(x + 2, 1 - c), 7)
    drain(6)
    drain(7)
    for cp in started:
        cp.wait_send()


def dispatch(n, le, cap, hidden, router_wt, ids_t):
    tokens, width = hidden.shape
    vm = pl.BlockSpec(memory_space=pltpu.VMEM)
    return pl.pallas_call(
        functools.partial(dispatch_kernel, n, le, cap),
        out_shape=(jax.ShapeDtypeStruct((le, n, cap, width), hidden.dtype),
                   jax.ShapeDtypeStruct((n, le * cap), jnp.int32),
                   jax.ShapeDtypeStruct((n, 128), jnp.int32),
                   jax.ShapeDtypeStruct((tokens, 128), F32)),
        in_specs=[vm, vm, vm],
        out_specs=(pl.BlockSpec(memory_space=pl.ANY), vm, vm, vm),
        scratch_shapes=[pltpu.VMEM((n, tokens, width), BF16), pltpu.VMEM((n, 2, tokens), jnp.int32),
                        pltpu.VMEM((2, le * cap, width), BF16), pltpu.SemaphoreType.DMA((PIECES * 7,)),
                        pltpu.SemaphoreType.DMA((3, PIECES)), pltpu.SemaphoreType.DMA((4, PIECES)),
                        pltpu.SemaphoreType.DMA((n, le)), pltpu.SemaphoreType.DMA((n,)),
                        pltpu.SemaphoreType.DMA((n,))],
        compiler_params=pltpu.CompilerParams(collective_id=1, has_side_effects=True,
                                             vmem_limit_bytes=40 * 1024 * 1024),
        name="dispatch",
    )(hidden, router_wt, ids_t)


DEPTH = 4
BLOCK = 512


def experts_kernel(n, le, cap, meta_ref, xs_ref, w1_ref, w3_ref, w2_ref, ys_ref, b1, b3, b2, x_buf, mid, acc, y_buf,
                   w_sem, x_sem, y_sem):
    width, ffn = w1_ref.shape[1:]
    steps = ffn // BLOCK
    total = le * steps

    def weights(s, act):
        l, f, k = s // steps, s % steps, s % DEPTH
        cols = pl.ds(pl.multiple_of(f * BLOCK, BLOCK), BLOCK)
        act(pltpu.make_async_copy(w1_ref.at[l, :, cols], b1.at[k], w_sem.at[k, 0]))
        act(pltpu.make_async_copy(w3_ref.at[l, :, cols], b3.at[k], w_sem.at[k, 1]))
        act(pltpu.make_async_copy(w2_ref.at[l, cols, :], b2.at[k], w_sem.at[k, 2]))

    def count16(i, l):
        return (meta_ref[i, l] + GRAN - 1) // GRAN

    def load_x(l):
        p = l % 2
        at = jnp.int32(0)
        for i in range(n):
            num = count16(i, l)
            for g in range(cap // GRAN):
                @pl.when(g < num)
                def _():
                    pltpu.make_async_copy(xs_ref.at[l, i, pl.ds(g * GRAN, GRAN)],
                                          x_buf.at[p, pl.ds(pl.multiple_of((at + g) * GRAN, GRAN), GRAN)],
                                          x_sem.at[p]).start()
            at = at + num
        x_buf[p, pl.ds(pl.multiple_of(at * GRAN, GRAN), TILE), :] = jnp.zeros((TILE, width), BF16)

    load_x(0)
    for s in range(DEPTH - 1):
        weights(jnp.int32(s), lambda cp: cp.start())

    def put_y(l, act):
        at = jnp.int32(0)
        for i in range(n):
            act(pltpu.make_async_copy(y_buf.at[l % 2, pl.ds(pl.multiple_of(at * GRAN, GRAN), cap)], ys_ref.at[l, i],
                                      y_sem.at[l % 2, i]))
            at = at + count16(i, l)

    def expert(l, carry):
        p = l % 2
        num = jnp.int32(0)
        for i in range(n):
            num = num + count16(i, l)

        def wait_x(_, carry):
            pltpu.make_async_copy(xs_ref.at[0, 0, pl.ds(0, GRAN)], x_buf.at[p, pl.ds(0, GRAN)], x_sem.at[p]).wait()
            return carry

        lax.fori_loop(0, num, wait_x, 0)

        @pl.when(l + 1 < le)
        def _():
            load_x(l + 1)

        @pl.when(l > 1)
        def _():
            put_y(l - 2, lambda cp: cp.wait())

        tiles = (num * GRAN + TILE - 1) // TILE

        def step(f, carry):
            s = l * steps + f
            k = s % DEPTH

            @pl.when(s + DEPTH - 1 < total)
            def _():
                weights(s + DEPTH - 1, lambda cp: cp.start())

            weights(s, lambda cp: cp.wait())

            def rows_of(start, rows):
                sl = pl.ds(pl.multiple_of(start, TILE), rows)
                xt = x_buf[p, sl, :]
                for j in range(BLOCK // 256):
                    cols = pl.ds(j * 256, 256)
                    a = jnp.dot(xt, b1[k, :, cols], preferred_element_type=F32)
                    b = jnp.dot(xt, b3[k, :, cols], preferred_element_type=F32)
                    mid[pl.ds(0, rows), cols] = (a * jax.nn.sigmoid(a) * b).astype(BF16)
                mt = mid[pl.ds(0, rows), :]
                for j in range(width // 512):
                    cols = pl.ds(j * 512, 512)
                    part = jnp.dot(mt, b2[k, :, cols], preferred_element_type=F32)
                    acc[sl, cols] = jnp.where(f == 0, 0.0, acc[sl, cols]) + part

            def pair(r, carry):
                rows_of(r * 2 * TILE, 2 * TILE)
                return carry

            lax.fori_loop(0, tiles // 2, pair, 0)

            @pl.when(tiles % 2 == 1)
            def _():
                rows_of((tiles - 1) * TILE, TILE)

            return carry

        lax.fori_loop(0, steps, step, 0)

        def finish(r, carry):
            sl = pl.ds(pl.multiple_of(r * TILE, TILE), TILE)
            y_buf[p, sl, :] = acc[sl, :].astype(BF16)
            return carry

        lax.fori_loop(0, tiles, finish, 0)
        y_buf[p, pl.ds(pl.multiple_of(tiles * TILE, TILE), cap), :] = jnp.zeros((cap, width), BF16)
        put_y(l, lambda cp: cp.start())
        return carry

    lax.fori_loop(0, le, expert, 0)
    for l in range(max(0, le - 2), le):
        put_y(jnp.int32(l), lambda cp: cp.wait())


def experts(n, le, cap, meta, xs, w_gate, w_up, w_down):
    width, ffn = w_gate.shape[1:]
    full = n * cap
    hbm = pl.BlockSpec(memory_space=pl.ANY)
    return pl.pallas_call(
        functools.partial(experts_kernel, n, le, cap),
        out_shape=jax.ShapeDtypeStruct((le, n, cap, width), BF16),
        in_specs=[pl.BlockSpec(memory_space=pltpu.SMEM), hbm, hbm, hbm, hbm],
        out_specs=hbm,
        scratch_shapes=[pltpu.VMEM((DEPTH, width, BLOCK), BF16), pltpu.VMEM((DEPTH, width, BLOCK), BF16),
                        pltpu.VMEM((DEPTH, BLOCK, width), BF16), pltpu.VMEM((2, full + TILE, width), BF16),
                        pltpu.VMEM((2 * TILE, BLOCK), BF16), pltpu.VMEM((full, width), F32),
                        pltpu.VMEM((2, full + cap, width), BF16), pltpu.SemaphoreType.DMA((DEPTH, 3)),
                        pltpu.SemaphoreType.DMA((2,)), pltpu.SemaphoreType.DMA((2, n))],
        compiler_params=pltpu.CompilerParams(vmem_limit_bytes=60 * 1024 * 1024),
        name="experts",
    )(meta, xs, w_gate, w_up, w_down)


def combine_kernel(n, le, cap, quota, post_ref, qmap_ref, comb_ref, h_ref, ys_ref, out_ref,
                   y_buf, mine, theirs, away, recv_buf, y_sem, pair_send, pair_recv, send_sem, recv_sem):
    ep = lax.axis_index("ep")
    chips = n // 2
    x, c = ep // 2, ep % 2
    pa = x * 2 + 1 - c
    bar = pltpu.get_barrier_semaphore()
    for o in range(1, n):
        pl.semaphore_signal(bar, inc=1, device_id={"ep": lax.rem(ep + o, n)}, device_id_type=MESH)

    order = [(2, 0), (2, 1), (1, 0), (3, 0), (1, 1), (3, 1), (0, 1), (0, 0)]
    dests = [lax.rem(x + dx, chips) * 2 + lax.rem(c + dc, 2) for dx, dc in order]

    def fetch(k):
        return pltpu.make_async_copy(ys_ref.at[:, dests[k]], y_buf.at[k % 2], y_sem.at[k % 2])

    fetch(0).start()
    fetch(1).start()
    pl.semaphore_wait(bar, n - 1)

    tokens, width = h_ref.shape
    row = lax.broadcasted_iota(jnp.int32, (quota, le * cap), 0)
    swaps, copies = [], []

    def pack(k):
        fetch(k).wait()
        slots = qmap_ref[pl.ds(dests[k], 1), :]
        rows = y_buf[k % 2].reshape(le * cap, width)
        away[k] = jnp.dot((slots - (1 - c) * quota == row).astype(F32).astype(BF16), rows,
                          preferred_element_type=F32).astype(BF16)
        cp = pltpu.make_async_remote_copy(src_ref=away.at[k], dst_ref=theirs.at[PARTNER[k]], send_sem=pair_send.at[k],
                                          recv_sem=pair_recv.at[PARTNER[k]], device_id={"ep": pa}, device_id_type=MESH)
        cp.start()
        swaps.append(cp)
        mine[k] = jnp.dot((slots - c * quota == row).astype(F32).astype(BF16), rows,
                          preferred_element_type=F32).astype(BF16)
        if k + 2 < n:
            fetch(k + 2).start()

    def send(k):
        swaps[PARTNER[k]].wait_recv()
        spot = pl.ds(pl.multiple_of(ep * quota, GRAN), quota)
        if k == n - 1:
            recv_buf[spot, :] = mine[k] + theirs[k]
            return
        mine[k] = mine[k] + theirs[k]
        cp = pltpu.make_async_remote_copy(src_ref=mine.at[k], dst_ref=recv_buf.at[spot], send_sem=send_sem.at[k],
                                          recv_sem=recv_sem.at[k], device_id={"ep": dests[k]}, device_id_type=MESH)
        cp.start()
        copies.append(cp)

    PARTNER = [order.index((dx, 1 - dc)) for dx, dc in order]
    pack(0)
    pack(1)
    pack(2)
    send(0)
    send(1)
    for k in range(3, n):
        pack(k)
        if k == 4:
            send(2)
        if k == 5:
            send(3)
            send(4)
    for k in range(5, n):
        send(k)

    pos0, pos1 = comb_ref[:, 0:1], comb_ref[:, 1:2]
    g0, g1 = comb_ref[:, 2:3], comb_ref[:, 3:4]
    pos0 = (comb_ref[:, 4:5] * (2 * quota) + pos0).astype(jnp.int32)
    pos1 = (comb_ref[:, 5:6] * (2 * quota) + pos1).astype(jnp.int32)
    lane = lax.broadcasted_iota(jnp.int32, (tokens, n * quota), 1)
    hot0 = (lane == pos0).astype(F32).astype(BF16)
    hot1 = (lane == pos1).astype(F32).astype(BF16)
    for cp in copies:
        cp.wait()
    for cp in swaps:
        cp.wait_send()
    alpha, beta = post_ref[0], post_ref[1]
    block = 512
    for d in range(width // block):
        cols = pl.ds(d * block, block)
        got = recv_buf[:, cols]
        y0 = jnp.dot(hot0, got, preferred_element_type=F32)
        y1 = jnp.dot(hot1, got, preferred_element_type=F32)
        mixed = g0 * y0 + g1 * y1
        out_ref[:, cols] = (alpha * h_ref[:, cols].astype(F32) + beta * mixed).astype(out_ref.dtype)


def combine(n, le, cap, quota, cid, post_scale, qmap, comb, hidden, ys):
    tokens, width = hidden.shape
    vm = pl.BlockSpec(memory_space=pltpu.VMEM)
    sm = pl.BlockSpec(memory_space=pltpu.SMEM)
    dma = pltpu.SemaphoreType.DMA
    part = pltpu.VMEM((n, quota, width), BF16)
    return pl.pallas_call(
        functools.partial(combine_kernel, n, le, cap, quota),
        out_shape=jax.ShapeDtypeStruct((tokens, width), hidden.dtype),
        in_specs=[sm, vm, vm, vm, pl.BlockSpec(memory_space=pl.ANY)],
        out_specs=vm,
        scratch_shapes=[pltpu.VMEM((2, le, cap, width), BF16), part, part, part,
                        pltpu.VMEM((n * quota, width), BF16), dma((2,)), dma((n,)), dma((n,)), dma((n,)), dma((n,))],
        compiler_params=pltpu.CompilerParams(collective_id=cid, has_side_effects=True,
                                             vmem_limit_bytes=60 * 1024 * 1024),
        name="combine%d" % quota,
    )(post_scale, qmap, comb, hidden, ys)


def solution(mesh):
    n = mesh.shape["ep"]

    def local_step(hidden, router_w, expert_ids, w_gate, w_up, w_down, post_scale):
        tokens, width = hidden.shape
        le = w_gate.shape[0]
        cap = tokens // max(1, (n * le) // 8)
        xs, qmap, meta, comb = dispatch(n, le, cap, hidden, router_w.T, expert_ids.T)
        ys = experts(n, le, cap, meta, xs, w_gate, w_up, w_down)
        quotas = [q for q in (96, 128) if q < le * cap] + [le * cap]
        worst = meta[0, le]
        branch = sum((worst > 2 * q).astype(jnp.int32) for q in quotas[:-1])
        return lax.switch(branch, [functools.partial(combine, n, le, cap, q, 2 + k) for k, q in enumerate(quotas)],
                          post_scale, qmap, comb, hidden, ys)

    tok = P(("dp", "ep"))
    return jax.shard_map(local_step, mesh=mesh, in_specs=(tok, P(), tok, P("ep"), P("ep"), P("ep"), P()),
                         out_specs=tok, check_vma=False)
```

```python
import functools

import jax
import jax.numpy as jnp
from jax import lax
from jax.experimental import pallas as pl
from jax.experimental.pallas import tpu as pltpu
from jax.sharding import PartitionSpec as P

MESH = pl.DeviceIdType.MESH
PIECES = 4
TILE = 128
GRAN = 16
BLOCK = 512
SLOTS = 5
COLS = 256
F32 = jnp.float32
BF16 = jnp.bfloat16


def dispatch_kernel(n, le, cap, h_hbm, wrt_hbm, idst_hbm, w1_ref, w3_ref, xs_ref, qmap_ref, meta_ref,
                    comb_ref, p1_ref, p3_ref, all_h, all_ids, h_ref, wrt_ref, idst_ref, send_sem, ring_sem, pair_sem,
                    in_sem, ids_send, ids_recv, w_sem):
    ep = lax.axis_index("ep")
    chips = n // 2
    x, c = ep // 2, ep % 2

    def dev(xx, cc):
        return lax.rem(xx + 2 * chips, chips) * 2 + cc

    xp, xm, pa = dev(x + 1, c), dev(x - 1, c), dev(x, 1 - c)
    inputs = [pltpu.make_async_copy(src, dst, in_sem.at[k])
              for k, (src, dst) in enumerate(((h_hbm, h_ref), (idst_hbm, idst_ref), (wrt_hbm, wrt_ref)))]
    for cp in inputs:
        cp.start()
    bar = pltpu.get_barrier_semaphore()
    for o in range(1, n):
        pl.semaphore_signal(bar, inc=1, device_id={"ep": lax.rem(ep + o, n)}, device_id_type=MESH)
    tokens, _ = h_ref.shape
    rows = tokens // PIECES
    started, loads = [], []
    inputs[0].wait()
    inputs[1].wait()
    pl.semaphore_wait(bar, n - 1)

    for o in range(1, n):
        cp = pltpu.make_async_remote_copy(
            src_ref=idst_ref, dst_ref=all_ids.at[ep], send_sem=ids_send.at[o], recv_sem=ids_recv.at[o],
            device_id={"ep": lax.rem(ep + o, n)}, device_id_type=MESH)
        cp.start()
        started.append(cp)
    own_ids = pltpu.make_async_copy(idst_ref, all_ids.at[ep], ids_recv.at[0])
    own_ids.start()

    count = [0]

    def push(src, blk, p, to, rsem):
        cp = pltpu.make_async_remote_copy(
            src_ref=src, dst_ref=all_h.at[blk, pl.ds(p * rows, rows)], send_sem=send_sem.at[count[0]], recv_sem=rsem,
            device_id={"ep": to}, device_id_type=MESH)
        count[0] += 1
        cp.start()
        started.append(cp)

    def arrive(blk, p, sem):
        ref = all_h.at[blk, pl.ds(p * rows, rows)]
        pltpu.make_async_remote_copy(src_ref=ref, dst_ref=ref, send_sem=send_sem.at[0], recv_sem=sem,
                                     device_id={"ep": pa}, device_id_type=MESH).wait_recv()

    last = PIECES - 1
    for s in range(PIECES):
        push(h_ref.at[pl.ds(s * rows, rows)], ep, s, xp, ring_sem.at[0, s])
        push(h_ref.at[pl.ds((last - s) * rows, rows)], ep, last - s, xm, ring_sem.at[1, last - s])
    for s in range(PIECES):
        push(h_ref.at[pl.ds(s * rows, rows)], ep, s, pa, pair_sem.at[0, s])

    steps = w1_ref.shape[2] // BLOCK
    for s in range(SLOTS):
        cols = pl.ds(s % steps * BLOCK, BLOCK)
        for k, (src, dst) in enumerate(((w1_ref, p1_ref), (w3_ref, p3_ref))):
            cp = pltpu.make_async_copy(src.at[s // steps, :, cols], dst.at[s], w_sem.at[s, k])
            cp.start()
            loads.append(cp)

    inputs[2].wait()
    own_ids.wait()
    for o in range(1, n):
        ref = all_ids.at[lax.rem(ep + n - o, n)]
        pltpu.make_async_remote_copy(src_ref=ref, dst_ref=ref, send_sem=ids_send.at[o], recv_sem=ids_recv.at[o],
                                     device_id={"ep": pa}, device_id_type=MESH).wait_recv()
    ids0 = all_ids[:, 0, :]
    ids1 = all_ids[:, 1, :]
    experts = n * le
    upper = (lax.broadcasted_iota(jnp.int32, (tokens, tokens), 0)
             < lax.broadcasted_iota(jnp.int32, (tokens, tokens), 1)).astype(F32).astype(BF16)

    def hits(lo, hi):
        return (jnp.where((ids0 >= lo) & (ids0 < hi), 1.0, 0.0) + jnp.where((ids1 >= lo) & (ids1 < hi), 1.0, 0.0))

    lane = lax.broadcasted_iota(jnp.int32, (n, le * cap), 1)
    lane_m = lax.broadcasted_iota(jnp.int32, meta_ref.shape, 1)
    qmap = jnp.full((n, le * cap), -1.0, F32)
    meta = jnp.zeros(meta_ref.shape, F32)
    offset = jnp.where(c > 0, 1.0, 0.0) * jnp.sum(hits(x * 2 * le, x * 2 * le + le), axis=1, keepdims=True)
    slots = []
    for l in range(le):
        e = ep * le + l
        mask = jnp.where((ids0 == e) | (ids1 == e), 1.0, 0.0)
        rank = jnp.dot(mask.astype(BF16), upper, preferred_element_type=F32)
        slots.append(jnp.where(mask > 0.5, rank, -1.0).astype(jnp.int32))
        cnt = jnp.sum(mask, axis=1, keepdims=True)
        inside = lane - l * cap
        insidef = inside.astype(F32)
        qmap = jnp.where((inside >= 0) & (inside < cap) & (insidef < cnt), offset + insidef, qmap)
        meta = jnp.where(lane_m == l, cnt, meta)
        offset = offset + cnt
    qmap_ref[...] = qmap.astype(jnp.int32)
    worst = jnp.zeros((n, 1), F32)
    for j in range(chips):
        worst = jnp.maximum(worst, jnp.sum(hits(j * 2 * le, (j + 1) * 2 * le), axis=1, keepdims=True))
    worst = jnp.max(worst, axis=0, keepdims=True)
    meta_ref[...] = jnp.where(lane_m == le, worst, meta).astype(jnp.int32)

    own0, own1 = idst_ref[0:1, :], idst_ref[1:2, :]
    sub = lax.broadcasted_iota(jnp.int32, (experts, tokens), 0)
    logits = lax.dot_general(wrt_ref[...], h_ref[...].astype(F32), (((1,), (1,)), ((), ())),
                             precision=lax.Precision.HIGHEST, preferred_element_type=F32)
    ex = jnp.exp(logits - jnp.max(logits, axis=0, keepdims=True))
    prob = ex / jnp.sum(ex, axis=0, keepdims=True)
    pick0, pick1 = sub == own0, sub == own1
    p0 = jnp.sum(jnp.where(pick0, prob, 0.0), axis=0, keepdims=True)
    p1 = jnp.sum(jnp.where(pick1, prob, 0.0), axis=0, keepdims=True)
    hot = jnp.where(pick0 | pick1, 1.0, 0.0)
    rank = jnp.dot(hot.astype(BF16), upper, preferred_element_type=F32)
    ei = lax.broadcasted_iota(jnp.int32, (experts, experts), 0)
    ej = lax.broadcasted_iota(jnp.int32, (experts, experts), 1)
    before = ((ei // (2 * le) == ej // (2 * le)) & (ej < ei)).astype(F32).astype(BF16)
    total = jnp.broadcast_to(jnp.sum(hot, axis=1, keepdims=True), (experts, 128)).astype(BF16)
    base = jnp.dot(before, total, preferred_element_type=F32)[:, 0:1]
    where = rank + base
    pos0 = jnp.sum(jnp.where(pick0, where, 0.0), axis=0, keepdims=True)
    pos1 = jnp.sum(jnp.where(pick1, where, 0.0), axis=0, keepdims=True)
    chip0, chip1 = (own0 // (2 * le)).astype(F32), (own1 // (2 * le)).astype(F32)
    row = lax.broadcasted_iota(jnp.int32, (128, tokens), 0)
    packed = jnp.zeros((128, tokens), F32)
    for k, v in enumerate((pos0, pos1, p0 / (p0 + p1), p1 / (p0 + p1), chip0, chip1)):
        packed = jnp.where(row == k, v, packed)
    comb_ref[...] = packed.T

    slot_row = lax.broadcasted_iota(jnp.int32, (cap, tokens), 0)

    def place(i, src):
        one_hot = []
        for l in range(le):
            one = slots[l]
            pick = jnp.sum(jnp.where(lax.broadcasted_iota(jnp.int32, one.shape, 0) == i, one, 0), axis=0, keepdims=True)
            one_hot.append((pick == slot_row).astype(F32).astype(BF16))
        one_hot = jnp.concatenate(one_hot, axis=0)
        half = src.shape[1] // 2
        for q in range(2):
            cols = pl.ds(q * half, half)
            got = jnp.dot(one_hot, src[:, cols], preferred_element_type=F32).astype(BF16)
            for l in range(le):
                xs_ref[l, i, :, cols] = got[l * cap:(l + 1) * cap]

    place(ep, h_ref)

    bm, bp, b2 = dev(x - 1, c), dev(x + 1, c), dev(x + 2, c)
    for s in range(PIECES):
        q = last - s
        arrive(bm, s, ring_sem.at[0, s])
        ref = all_h.at[bm, pl.ds(s * rows, rows)]
        if s < PIECES // 2:
            push(ref, bm, s, xp, ring_sem.at[2, s])
        push(ref, bm, s, pa, pair_sem.at[1, s])
        arrive(bp, q, ring_sem.at[1, q])
        ref = all_h.at[bp, pl.ds(q * rows, rows)]
        if s < PIECES // 2:
            push(ref, bp, q, xm, ring_sem.at[2, q])
        push(ref, bp, q, pa, pair_sem.at[2, q])
    def landed(i, xx):
        for s in range(PIECES):
            arrive(dev(xx, 1 - c), s, pair_sem.at[i, s])

    landed(0, x)
    place(pa, all_h.at[pa])
    place(bm, all_h.at[bm])
    place(bp, all_h.at[bp])
    for k, xx in enumerate((x - 1, x + 1)):
        landed(1 + k, xx)
        place(dev(xx, 1 - c), all_h.at[dev(xx, 1 - c)])
    for r in range(PIECES // 2):
        for q in (r, last - r):
            arrive(b2, q, ring_sem.at[2, q])
            push(all_h.at[b2, pl.ds(q * rows, rows)], b2, q, pa, pair_sem.at[3, q])
    place(b2, all_h.at[b2])
    landed(3, x + 2)
    place(dev(x + 2, 1 - c), all_h.at[dev(x + 2, 1 - c)])
    for cp in started:
        cp.wait_send()
    for cp in loads:
        cp.wait()


def dispatch(n, le, cap, hidden, router_wt, ids_t, w_gate, w_up):
    tokens, width = hidden.shape
    vm = pl.BlockSpec(memory_space=pltpu.VMEM)
    hbm = pl.BlockSpec(memory_space=pltpu.HBM)
    dma = pltpu.SemaphoreType.DMA
    ring = jax.ShapeDtypeStruct((SLOTS, width, BLOCK), BF16)
    return pl.pallas_call(
        functools.partial(dispatch_kernel, n, le, cap),
        out_shape=(jax.ShapeDtypeStruct((le, n, cap, width), hidden.dtype),
                   jax.ShapeDtypeStruct((n, le * cap), jnp.int32),
                   jax.ShapeDtypeStruct((n, 128), jnp.int32),
                   jax.ShapeDtypeStruct((tokens, 128), F32), ring, ring),
        in_specs=[hbm, hbm, hbm, hbm, hbm],
        out_specs=(vm, vm, vm, vm, vm, vm),
        scratch_shapes=[pltpu.VMEM((n, tokens, width), BF16), pltpu.VMEM((n, 2, tokens), jnp.int32),
                        pltpu.VMEM((tokens, width), BF16), pltpu.VMEM(router_wt.shape, F32),
                        pltpu.VMEM(ids_t.shape, jnp.int32), dma((PIECES * 7,)), dma((3, PIECES)), dma((4, PIECES)),
                        dma((3,)), dma((n,)), dma((n,)), dma((SLOTS, 2))],
        compiler_params=pltpu.CompilerParams(collective_id=1, has_side_effects=True,
                                             vmem_limit_bytes=20 * 1024 * 1024),
        name="dispatch",
    )(*[pltpu.with_memory_space_constraint(a, pltpu.HBM) for a in (hidden, router_wt, ids_t, w_gate, w_up)])


def experts_kernel(n, le, cap, meta_ref, xs_ref, w1_ref, w3_ref, _p1, _p3, ms_ref, b1, b3, x_buf, m_buf, w_sem, x_sem,
                   m_sem):
    width, ffn = w1_ref.shape[1:]
    steps = ffn // BLOCK
    total = le * steps
    full = n * cap

    def weights(s, act):
        l, f, k = s // steps, s % steps, s % SLOTS
        cols = pl.ds(pl.multiple_of(f * BLOCK, BLOCK), BLOCK)
        act(pltpu.make_async_copy(w1_ref.at[l, :, cols], b1.at[k], w_sem.at[k, 0]))
        act(pltpu.make_async_copy(w3_ref.at[l, :, cols], b3.at[k], w_sem.at[k, 1]))

    def count16(i, l):
        return (meta_ref[i, l] + GRAN - 1) // GRAN

    def load_x(l):
        p = l % 2
        at = jnp.int32(0)
        for i in range(n):
            num = count16(i, l)
            for g in range(cap // GRAN):
                @pl.when(g < num)
                def _():
                    pltpu.make_async_copy(xs_ref.at[l, i, pl.ds(g * GRAN, GRAN)],
                                          x_buf.at[p, pl.ds(pl.multiple_of((at + g) * GRAN, GRAN), GRAN)],
                                          x_sem.at[p]).start()
            at = at + num
        x_buf[p, pl.ds(pl.multiple_of(at * GRAN, GRAN), TILE), :] = jnp.zeros((TILE, width), BF16)

    load_x(0)

    def put_m(l, act):
        at = jnp.int32(0)
        for i in range(n):
            act(pltpu.make_async_copy(m_buf.at[l % 2, pl.ds(pl.multiple_of(at * GRAN, GRAN), cap)], ms_ref.at[l, pl.ds(i * cap, cap)],
                                      m_sem.at[l % 2, i]))
            at = at + count16(i, l)

    def expert(l, carry):
        p = l % 2
        num = jnp.int32(0)
        for i in range(n):
            num = num + count16(i, l)

        def wait_x(_, carry):
            pltpu.make_async_copy(xs_ref.at[0, 0, pl.ds(0, GRAN)], x_buf.at[p, pl.ds(0, GRAN)], x_sem.at[p]).wait()
            return carry

        lax.fori_loop(0, num, wait_x, 0)

        @pl.when(l + 1 < le)
        def _():
            load_x(l + 1)

        @pl.when(l > 1)
        def _():
            put_m(l - 2, lambda cp: cp.wait())

        tiles = (num * GRAN + TILE - 1) // TILE

        def step(f, carry):
            s = l * steps + f
            k = s % SLOTS

            @pl.when((s > 0) & (s + SLOTS - 1 < total))
            def _():
                weights(s + SLOTS - 1, lambda cp: cp.start())

            @pl.when(s >= SLOTS)
            def _():
                weights(s, lambda cp: cp.wait())

            def rows_of(rows):
                sl = pl.ds(0, rows)
                xt = x_buf[p, sl, :]
                for j in range(BLOCK // 256):
                    cols = pl.ds(j * 256, 256)
                    a = jnp.dot(xt, b1[k, :, cols], preferred_element_type=F32)
                    b = jnp.dot(xt, b3[k, :, cols], preferred_element_type=F32)
                    m_buf[p, sl, pl.ds(pl.multiple_of(f * BLOCK + j * 256, 256), 256)] = (
                        a * jax.nn.sigmoid(a) * b).astype(BF16)

            for t in range(1, full // TILE + 1):
                @pl.when(tiles == t)
                def _():
                    rows_of(t * TILE)

            return carry

        lax.fori_loop(0, steps, step, 0)
        m_buf[p, pl.ds(pl.multiple_of(tiles * TILE, TILE), cap), :] = jnp.zeros((cap, ffn), BF16)
        put_m(l, lambda cp: cp.start())
        return carry

    lax.fori_loop(0, le, expert, 0)
    for l in range(max(0, le - 2), le):
        put_m(jnp.int32(l), lambda cp: cp.wait())


def experts(n, le, cap, meta, xs, w_gate, w_up, p1, p3):
    width, ffn = w_gate.shape[1:]
    full = n * cap
    hbm = pl.BlockSpec(memory_space=pltpu.HBM)
    vm = pl.BlockSpec(memory_space=pltpu.VMEM)
    dma = pltpu.SemaphoreType.DMA
    return pl.pallas_call(
        functools.partial(experts_kernel, n, le, cap),
        out_shape=(jax.ShapeDtypeStruct((le, full, ffn), BF16), jax.ShapeDtypeStruct(p1.shape, BF16),
                   jax.ShapeDtypeStruct(p3.shape, BF16)),
        in_specs=[pl.BlockSpec(memory_space=pltpu.SMEM), vm, hbm, hbm, vm, vm],
        out_specs=(vm, vm, vm),
        input_output_aliases={4: 1, 5: 2},
        scratch_shapes=[pltpu.VMEM((2, full + TILE, width), BF16), pltpu.VMEM((2, full + cap, ffn), BF16),
                        dma((SLOTS, 2)), dma((2,)), dma((2, n))],
        compiler_params=pltpu.CompilerParams(vmem_limit_bytes=18 * 1024 * 1024),
        name="experts",
    )(meta, xs, w_gate, w_up, p1, p3)[0]


def combine_kernel(n, le, cap, quota, post_ref, qmap_ref, comb_ref, h_ref, ms_ref, w2_ref, out_ref,
                   ring, y_buf, spread, mine, theirs, away, recv_buf, gather0, gather1, w_sem, pair_send, pair_recv,
                   send_sem, recv_sem):
    ep = lax.axis_index("ep")
    chips = n // 2
    x, c = ep // 2, ep % 2
    pa = x * 2 + 1 - c
    bar = pltpu.get_barrier_semaphore()
    for o in range(1, n):
        pl.semaphore_signal(bar, inc=1, device_id={"ep": lax.rem(ep + o, n)}, device_id_type=MESH)

    tokens, width = h_ref.shape
    chunks = width // COLS

    def weights(d, l):
        cols = pl.ds(pl.multiple_of(d * COLS, COLS), COLS)
        return pltpu.make_async_copy(w2_ref.at[l, :, cols], ring.at[lax.rem(d, 2), l], w_sem.at[lax.rem(d, 2), l])

    for d in range(2):
        for l in range(le):
            weights(jnp.int32(d), l).start()

    order = [(2, 0), (2, 1), (1, 0), (3, 0), (1, 1), (3, 1), (0, 1), (0, 0)]
    partner = [order.index((dx, 1 - dc)) for dx, dc in order]
    dests = [lax.rem(x + dx, chips) * 2 + lax.rem(c + dc, 2) for dx, dc in order]
    spot = pl.ds(pl.multiple_of(ep * quota, GRAN), quota)

    row = lax.broadcasted_iota(jnp.int32, (quota, le * cap), 0)
    for k in range(n):
        slots = qmap_ref[pl.ds(dests[k], 1), :]
        spread[k, pl.ds(0, quota), :] = (slots - c * quota == row).astype(F32).astype(BF16)
        spread[k, pl.ds(quota, quota), :] = (slots - (1 - c) * quota == row).astype(F32).astype(BF16)

    def swap(d, k):
        return pltpu.make_async_remote_copy(
            src_ref=away.at[lax.rem(d, 2), k], dst_ref=theirs.at[d, partner[k]], send_sem=pair_send.at[lax.rem(d, 2), k],
            recv_sem=pair_recv.at[d, partner[k]], device_id={"ep": pa}, device_id_type=MESH)

    def push(d, k):
        return pltpu.make_async_remote_copy(
            src_ref=mine.at[d, k], dst_ref=recv_buf.at[d, spot], send_sem=send_sem.at[d, k], recv_sem=recv_sem.at[d, k],
            device_id={"ep": dests[k]}, device_id_type=MESH)

    def send(d):
        for k in range(n):
            swap(d, partner[k]).wait_recv()
            if k == n - 1:
                recv_buf[d, spot, :] = mine[d, k] + theirs[d, k]
            else:
                mine[d, k] = mine[d, k] + theirs[d, k]
                push(d, k).start()

    def project(d, some):
        for l in some:
            weights(d, l).wait()
        for l in some:
            y = jnp.dot(ms_ref[l], ring[lax.rem(d, 2), l], preferred_element_type=F32)
            y_buf[:, pl.ds(l * cap, cap), :] = y.astype(BF16).reshape(n, cap, COLS)

    def chunk(d, carry):
        @pl.when(d > 1)
        def _():
            send(d - 1)

        project(d, range(le // 2, le))

        @pl.when(d + 2 < chunks)
        def _():
            for l in range(le):
                weights(d + 2, l).start()

        @pl.when(d > 1)
        def _():
            for k in range(n):
                swap(d - 2, k).wait_send()

        for k in range(n):
            both = jnp.dot(spread[k], y_buf[dests[k]], preferred_element_type=F32).astype(BF16)
            away[lax.rem(d, 2), k] = both[quota:]
            mine[d, k] = both[:quota]
        for k in range(n):
            swap(d, k).start()

        @pl.when(d == 0)
        def _():
            send(d)

        @pl.when(d + 1 < chunks)
        def _():
            project(d + 1, range(le // 2))

        return carry

    project(jnp.int32(0), range(le // 2))
    pl.semaphore_wait(bar, n - 1)
    lax.fori_loop(0, chunks, chunk, 0)
    send(jnp.int32(chunks - 1))

    def tables(r, carry):
        some = pl.ds(pl.multiple_of(r * 32, 32), 32)
        lane = lax.broadcasted_iota(jnp.int32, (32, n * quota), 1)
        for k, table in enumerate((gather0, gather1)):
            pos = (comb_ref[some, 4 + k:5 + k] * (2 * quota) + comb_ref[some, k:k + 1]).astype(jnp.int32)
            table[some, :] = (lane == pos).astype(F32).astype(BF16)
        return carry

    lax.fori_loop(0, tokens // 32, tables, 0)
    g0, g1 = comb_ref[:, 2:3], comb_ref[:, 3:4]
    alpha, beta = post_ref[0], post_ref[1]

    def finish(d, carry):
        for k in range(n - 1):
            push(d, k).wait_recv()
        cols = pl.ds(pl.multiple_of(d * COLS, COLS), COLS)
        got = recv_buf[d]
        y0 = jnp.dot(gather0[...], got, preferred_element_type=F32)
        y1 = jnp.dot(gather1[...], got, preferred_element_type=F32)
        mixed = g0 * y0 + g1 * y1
        out_ref[:, cols] = (alpha * h_ref[:, cols].astype(F32) + beta * mixed).astype(out_ref.dtype)
        for k in range(n - 1):
            push(d, k).wait_send()
        return carry

    lax.fori_loop(0, chunks, finish, 0)
    for d in range(chunks - 2, chunks):
        for k in range(n):
            swap(jnp.int32(d), k).wait_send()


def combine(n, le, cap, quota, cid, post_scale, qmap, comb, hidden, ms, w_down):
    tokens, width = hidden.shape
    ffn = ms.shape[2]
    vm = pl.BlockSpec(memory_space=pltpu.VMEM)
    sm = pl.BlockSpec(memory_space=pltpu.SMEM)
    dma = pltpu.SemaphoreType.DMA
    chunks = width // COLS
    part = pltpu.VMEM((chunks, n, quota, COLS), BF16)
    table = pltpu.VMEM((tokens, n * quota), BF16)
    return pl.pallas_call(
        functools.partial(combine_kernel, n, le, cap, quota),
        out_shape=jax.ShapeDtypeStruct((tokens, width), hidden.dtype),
        in_specs=[sm, vm, vm, vm, vm, pl.BlockSpec(memory_space=pltpu.HBM)],
        out_specs=vm,
        scratch_shapes=[pltpu.VMEM((2, le, ffn, COLS), BF16), pltpu.VMEM((n, le * cap, COLS), BF16),
                        pltpu.VMEM((n, 2 * quota, le * cap), BF16), part, part,
                        pltpu.VMEM((2, n, quota, COLS), BF16), pltpu.VMEM((chunks, n * quota, COLS), BF16), table, table,
                        dma((2, le)), dma((2, n)), dma((chunks, n)), dma((chunks, n)), dma((chunks, n))],
        compiler_params=pltpu.CompilerParams(collective_id=cid, has_side_effects=True,
                                             vmem_limit_bytes=(36 if quota <= 128 else 49) * 1024 * 1024),
        name="combine%d" % quota,
    )(post_scale, qmap, comb, hidden, ms, w_down)


def solution(mesh):
    n = mesh.shape["ep"]

    def local_step(hidden, router_w, expert_ids, w_gate, w_up, w_down, post_scale):
        tokens, width = hidden.shape
        le = w_gate.shape[0]
        cap = tokens // max(1, (n * le) // 8)
        xs, qmap, meta, comb, p1, p3 = dispatch(n, le, cap, hidden, router_w.T, expert_ids.T, w_gate, w_up)
        ms = experts(n, le, cap, meta, xs, w_gate, w_up, p1, p3)
        quotas = [q for q in (96, 128) if q < le * cap] + [le * cap]
        worst = meta[0, le]
        branch = sum((worst > 2 * q).astype(jnp.int32) for q in quotas[:-1])
        return lax.switch(branch, [functools.partial(combine, n, le, cap, q, 2 + k) for k, q in enumerate(quotas)],
                          post_scale, qmap, comb, hidden, ms, w_down)

    tok = P(("dp", "ep"))
    return jax.shard_map(local_step, mesh=mesh, in_specs=(tok, P(), tok, P("ep"), P("ep"), P("ep"), P()),
                         out_specs=tok, check_vma=False)
```

```python
import functools

import jax
import jax.numpy as jnp
from jax import lax
from jax.experimental import pallas as pl
from jax.experimental.pallas import tpu as pltpu
from jax.sharding import PartitionSpec as P

MESH = pl.DeviceIdType.MESH
PIECES = 4
GRAN = 16
BLOCK = 512
SLOTS = 6
COLS = 256
F32 = jnp.float32
BF16 = jnp.bfloat16


def dispatch_kernel(n, le, cap, h_hbm, wrt_hbm, idst_hbm, w1_ref, w3_ref, xs_ref, qmap_ref, meta_ref,
                    comb_ref, p1_ref, p3_ref, all_h, all_ids, h_ref, wrt_ref, idst_ref, send_sem, ring_sem, pair_sem,
                    in_sem, ids_send, ids_recv, w_sem):
    ep = lax.axis_index("ep")
    chips = n // 2
    x, c = ep // 2, ep % 2

    def dev(xx, cc):
        return lax.rem(xx + 2 * chips, chips) * 2 + cc

    xp, xm, pa = dev(x + 1, c), dev(x - 1, c), dev(x, 1 - c)
    inputs = [pltpu.make_async_copy(src, dst, in_sem.at[k])
              for k, (src, dst) in enumerate(((h_hbm, h_ref), (idst_hbm, idst_ref), (wrt_hbm, wrt_ref)))]
    for cp in inputs:
        cp.start()
    bar = pltpu.get_barrier_semaphore()
    for o in range(1, n):
        pl.semaphore_signal(bar, inc=1, device_id={"ep": lax.rem(ep + o, n)}, device_id_type=MESH)
    tokens, _ = h_ref.shape
    rows = tokens // PIECES
    started, loads = [], []
    inputs[0].wait()
    inputs[1].wait()
    pl.semaphore_wait(bar, n - 1)

    for o in range(1, n):
        cp = pltpu.make_async_remote_copy(
            src_ref=idst_ref, dst_ref=all_ids.at[ep], send_sem=ids_send.at[o], recv_sem=ids_recv.at[o],
            device_id={"ep": lax.rem(ep + o, n)}, device_id_type=MESH)
        cp.start()
        started.append(cp)
    own_ids = pltpu.make_async_copy(idst_ref, all_ids.at[ep], ids_recv.at[0])
    own_ids.start()

    count = [0]

    def push(src, blk, p, to, rsem):
        cp = pltpu.make_async_remote_copy(
            src_ref=src, dst_ref=all_h.at[blk, pl.ds(p * rows, rows)], send_sem=send_sem.at[count[0]], recv_sem=rsem,
            device_id={"ep": to}, device_id_type=MESH)
        count[0] += 1
        cp.start()
        started.append(cp)

    def arrive(blk, p, sem):
        ref = all_h.at[blk, pl.ds(p * rows, rows)]
        pltpu.make_async_remote_copy(src_ref=ref, dst_ref=ref, send_sem=send_sem.at[0], recv_sem=sem,
                                     device_id={"ep": pa}, device_id_type=MESH).wait_recv()

    last = PIECES - 1
    for s in range(PIECES):
        push(h_ref.at[pl.ds(s * rows, rows)], ep, s, xp, ring_sem.at[0, s])
        push(h_ref.at[pl.ds((last - s) * rows, rows)], ep, last - s, xm, ring_sem.at[1, last - s])
    for s in range(PIECES):
        push(h_ref.at[pl.ds(s * rows, rows)], ep, s, pa, pair_sem.at[0, s])

    steps = w1_ref.shape[2] // BLOCK
    for s in range(SLOTS):
        cols = pl.ds(s % steps * BLOCK, BLOCK)
        for k, (src, dst) in enumerate(((w1_ref, p1_ref), (w3_ref, p3_ref))):
            cp = pltpu.make_async_copy(src.at[s // steps, :, cols], dst.at[s], w_sem.at[s, k])
            cp.start()
            loads.append(cp)

    inputs[2].wait()
    own_ids.wait()
    for o in range(1, n):
        ref = all_ids.at[lax.rem(ep + n - o, n)]
        pltpu.make_async_remote_copy(src_ref=ref, dst_ref=ref, send_sem=ids_send.at[o], recv_sem=ids_recv.at[o],
                                     device_id={"ep": pa}, device_id_type=MESH).wait_recv()
    ids0 = all_ids[:, 0, :]
    ids1 = all_ids[:, 1, :]
    experts = n * le
    upper = (lax.broadcasted_iota(jnp.int32, (tokens, tokens), 0)
             < lax.broadcasted_iota(jnp.int32, (tokens, tokens), 1)).astype(F32).astype(BF16)

    def hits(lo, hi):
        return (jnp.where((ids0 >= lo) & (ids0 < hi), 1.0, 0.0) + jnp.where((ids1 >= lo) & (ids1 < hi), 1.0, 0.0))

    lane = lax.broadcasted_iota(jnp.int32, (n, le * cap), 1)
    lane_m = lax.broadcasted_iota(jnp.int32, meta_ref.shape, 1)
    qmap = jnp.full((n, le * cap), -1.0, F32)
    meta = jnp.zeros(meta_ref.shape, F32)
    offset = jnp.where(c > 0, 1.0, 0.0) * jnp.sum(hits(x * 2 * le, x * 2 * le + le), axis=1, keepdims=True)
    slots = []
    for l in range(le):
        e = ep * le + l
        mask = jnp.where((ids0 == e) | (ids1 == e), 1.0, 0.0)
        rank = jnp.dot(mask.astype(BF16), upper, preferred_element_type=F32)
        slots.append(jnp.where(mask > 0.5, rank, -1.0).astype(jnp.int32))
        cnt = jnp.sum(mask, axis=1, keepdims=True)
        inside = lane - l * cap
        insidef = inside.astype(F32)
        qmap = jnp.where((inside >= 0) & (inside < cap) & (insidef < cnt), offset + insidef, qmap)
        meta = jnp.where(lane_m == l, cnt, meta)
        offset = offset + cnt
    qmap_ref[...] = qmap.astype(jnp.int32)
    worst = jnp.zeros((n, 1), F32)
    for j in range(chips):
        worst = jnp.maximum(worst, jnp.sum(hits(j * 2 * le, (j + 1) * 2 * le), axis=1, keepdims=True))
    worst = jnp.max(worst, axis=0, keepdims=True)
    meta_ref[...] = jnp.where(lane_m == le, worst, meta).astype(jnp.int32)

    own0, own1 = idst_ref[0:1, :], idst_ref[1:2, :]
    sub = lax.broadcasted_iota(jnp.int32, (experts, tokens), 0)
    logits = lax.dot_general(wrt_ref[...], h_ref[...].astype(F32), (((1,), (1,)), ((), ())),
                             precision=lax.Precision.HIGHEST, preferred_element_type=F32)
    ex = jnp.exp(logits - jnp.max(logits, axis=0, keepdims=True))
    prob = ex / jnp.sum(ex, axis=0, keepdims=True)
    pick0, pick1 = sub == own0, sub == own1
    p0 = jnp.sum(jnp.where(pick0, prob, 0.0), axis=0, keepdims=True)
    p1 = jnp.sum(jnp.where(pick1, prob, 0.0), axis=0, keepdims=True)
    hot = jnp.where(pick0 | pick1, 1.0, 0.0)
    rank = jnp.dot(hot.astype(BF16), upper, preferred_element_type=F32)
    ei = lax.broadcasted_iota(jnp.int32, (experts, experts), 0)
    ej = lax.broadcasted_iota(jnp.int32, (experts, experts), 1)
    before = ((ei // (2 * le) == ej // (2 * le)) & (ej < ei)).astype(F32).astype(BF16)
    total = jnp.broadcast_to(jnp.sum(hot, axis=1, keepdims=True), (experts, 128)).astype(BF16)
    base = jnp.dot(before, total, preferred_element_type=F32)[:, 0:1]
    where = rank + base
    pos0 = jnp.sum(jnp.where(pick0, where, 0.0), axis=0, keepdims=True)
    pos1 = jnp.sum(jnp.where(pick1, where, 0.0), axis=0, keepdims=True)
    chip0, chip1 = (own0 // (2 * le)).astype(F32), (own1 // (2 * le)).astype(F32)
    row = lax.broadcasted_iota(jnp.int32, (128, tokens), 0)
    packed = jnp.zeros((128, tokens), F32)
    for k, v in enumerate((pos0, pos1, p0 / (p0 + p1), p1 / (p0 + p1), chip0, chip1)):
        packed = jnp.where(row == k, v, packed)
    comb_ref[...] = packed.T

    slot_row = lax.broadcasted_iota(jnp.int32, (cap, tokens), 0)

    def place(i, src):
        one_hot = []
        for l in range(le):
            one = slots[l]
            pick = jnp.sum(jnp.where(lax.broadcasted_iota(jnp.int32, one.shape, 0) == i, one, 0), axis=0, keepdims=True)
            one_hot.append((pick == slot_row).astype(F32).astype(BF16))
        one_hot = jnp.concatenate(one_hot, axis=0)
        half = src.shape[1] // 2
        for q in range(2):
            cols = pl.ds(q * half, half)
            got = jnp.dot(one_hot, src[:, cols], preferred_element_type=F32).astype(BF16)
            for l in range(le):
                xs_ref[l, pl.ds(pl.multiple_of(i * cap, cap), cap), cols] = got[l * cap:(l + 1) * cap]

    place(ep, h_ref)

    bm, bp, b2 = dev(x - 1, c), dev(x + 1, c), dev(x + 2, c)
    for s in range(PIECES):
        q = last - s
        arrive(bm, s, ring_sem.at[0, s])
        ref = all_h.at[bm, pl.ds(s * rows, rows)]
        if s < PIECES // 2:
            push(ref, bm, s, xp, ring_sem.at[2, s])
        push(ref, bm, s, pa, pair_sem.at[1, s])
        arrive(bp, q, ring_sem.at[1, q])
        ref = all_h.at[bp, pl.ds(q * rows, rows)]
        if s < PIECES // 2:
            push(ref, bp, q, xm, ring_sem.at[2, q])
        push(ref, bp, q, pa, pair_sem.at[2, q])
    def landed(i, xx):
        for s in range(PIECES):
            arrive(dev(xx, 1 - c), s, pair_sem.at[i, s])

    landed(0, x)
    place(pa, all_h.at[pa])
    place(bm, all_h.at[bm])
    place(bp, all_h.at[bp])
    for k, xx in enumerate((x - 1, x + 1)):
        landed(1 + k, xx)
        place(dev(xx, 1 - c), all_h.at[dev(xx, 1 - c)])
    for r in range(PIECES // 2):
        for q in (r, last - r):
            arrive(b2, q, ring_sem.at[2, q])
            push(all_h.at[b2, pl.ds(q * rows, rows)], b2, q, pa, pair_sem.at[3, q])
    place(b2, all_h.at[b2])
    landed(3, x + 2)
    place(dev(x + 2, 1 - c), all_h.at[dev(x + 2, 1 - c)])
    for cp in started:
        cp.wait_send()
    for cp in loads:
        cp.wait()


def dispatch(n, le, cap, hidden, router_wt, ids_t, w_gate, w_up):
    tokens, width = hidden.shape
    vm = pl.BlockSpec(memory_space=pltpu.VMEM)
    hbm = pl.BlockSpec(memory_space=pltpu.HBM)
    dma = pltpu.SemaphoreType.DMA
    ring = jax.ShapeDtypeStruct((SLOTS, width, BLOCK), BF16)
    return pl.pallas_call(
        functools.partial(dispatch_kernel, n, le, cap),
        out_shape=(jax.ShapeDtypeStruct((le, n * cap, width), hidden.dtype),
                   jax.ShapeDtypeStruct((n, le * cap), jnp.int32),
                   jax.ShapeDtypeStruct((n, 128), jnp.int32),
                   jax.ShapeDtypeStruct((tokens, 128), F32), ring, ring),
        in_specs=[hbm, hbm, hbm, hbm, hbm],
        out_specs=(vm, vm, vm, vm, vm, vm),
        scratch_shapes=[pltpu.VMEM((n, tokens, width), BF16), pltpu.VMEM((n, 2, tokens), jnp.int32),
                        pltpu.VMEM((tokens, width), BF16), pltpu.VMEM(router_wt.shape, F32),
                        pltpu.VMEM(ids_t.shape, jnp.int32), dma((PIECES * 7,)), dma((3, PIECES)), dma((4, PIECES)),
                        dma((3,)), dma((n,)), dma((n,)), dma((SLOTS, 2))],
        compiler_params=pltpu.CompilerParams(collective_id=1, has_side_effects=True,
                                             vmem_limit_bytes=16 * 1024 * 1024),
        name="dispatch",
    )(*[pltpu.with_memory_space_constraint(a, pltpu.HBM) for a in (hidden, router_wt, ids_t, w_gate, w_up)])


def experts_kernel(n, le, cap, meta_ref, xs_ref, w1_ref, w3_ref, _p1, _p3, ms_ref, b1, b3, x_buf, w_sem):
    width, ffn = w1_ref.shape[1:]
    steps = ffn // BLOCK
    total = le * steps

    def weights(s, act):
        l, f, k = s // steps, s % steps, s % SLOTS
        cols = pl.ds(pl.multiple_of(f * BLOCK, BLOCK), BLOCK)
        act(pltpu.make_async_copy(w1_ref.at[l, :, cols], b1.at[k], w_sem.at[k, 0]))
        act(pltpu.make_async_copy(w3_ref.at[l, :, cols], b3.at[k], w_sem.at[k, 1]))

    def run(l, part):
        rows = n * part
        if part < cap:
            for i in range(n):
                x_buf[pl.ds(i * part, part), :] = xs_ref[l, pl.ds(i * cap, part), :]
                ms_ref[l, pl.ds(i * cap + part, cap - part), :] = jnp.zeros((cap - part, ffn), BF16)

        def step(f, carry):
            s = l * steps + f
            k = s % SLOTS

            @pl.when((s > 0) & (s + SLOTS - 1 < total))
            def _():
                weights(s + SLOTS - 1, lambda cp: cp.start())

            @pl.when(s >= SLOTS)
            def _():
                weights(s, lambda cp: cp.wait())

            xt = x_buf[pl.ds(0, rows), :] if part < cap else xs_ref[l]
            for j in range(BLOCK // 256):
                cols = pl.ds(j * 256, 256)
                a = jnp.dot(xt, b1[k, :, cols], preferred_element_type=F32)
                b = jnp.dot(xt, b3[k, :, cols], preferred_element_type=F32)
                mid = (a * jax.nn.sigmoid(a) * b).astype(BF16)
                out = pl.ds(pl.multiple_of(f * BLOCK + j * 256, 256), 256)
                if part < cap:
                    for i in range(n):
                        ms_ref[l, pl.ds(i * cap, part), out] = mid[i * part:(i + 1) * part]
                else:
                    ms_ref[l, :, out] = mid
            return carry

        lax.fori_loop(0, steps, step, 0)

    def expert(l, carry):
        most = meta_ref[0, l]
        for i in range(1, n):
            most = jnp.maximum(most, meta_ref[i, l])
        parts = (GRAN, 2 * GRAN, cap)
        for k, part in enumerate(parts):
            low = parts[k - 1] if k else -1
            high = part if part < cap else n * cap

            @pl.when((most > low) & (most <= high))
            def _():
                run(l, part)

        return carry

    lax.fori_loop(0, le, expert, 0)


def experts(n, le, cap, meta, xs, w_gate, w_up, p1, p3):
    width, ffn = w_gate.shape[1:]
    full = n * cap
    hbm = pl.BlockSpec(memory_space=pltpu.HBM)
    vm = pl.BlockSpec(memory_space=pltpu.VMEM)
    dma = pltpu.SemaphoreType.DMA
    return pl.pallas_call(
        functools.partial(experts_kernel, n, le, cap),
        out_shape=(jax.ShapeDtypeStruct((le, full, ffn), BF16), jax.ShapeDtypeStruct(p1.shape, BF16),
                   jax.ShapeDtypeStruct(p3.shape, BF16)),
        in_specs=[pl.BlockSpec(memory_space=pltpu.SMEM), vm, hbm, hbm, vm, vm],
        out_specs=(vm, vm, vm),
        input_output_aliases={4: 1, 5: 2},
        scratch_shapes=[pltpu.VMEM((n * 2 * GRAN, width), BF16), dma((SLOTS, 2))],
        compiler_params=pltpu.CompilerParams(vmem_limit_bytes=8 * 1024 * 1024),
        name="experts",
    )(meta, xs, w_gate, w_up, p1, p3)[0]


def combine_kernel(n, le, cap, quota, post_ref, qmap_ref, comb_ref, h_ref, ms_ref, w2_ref, out_ref,
                   ring, y_buf, spread, mine, theirs, away, recv_buf, gather0, gather1, w_sem, pair_send, pair_recv,
                   send_sem, recv_sem):
    ep = lax.axis_index("ep")
    chips = n // 2
    x, c = ep // 2, ep % 2
    pa = x * 2 + 1 - c
    bar = pltpu.get_barrier_semaphore()
    for o in range(1, n):
        pl.semaphore_signal(bar, inc=1, device_id={"ep": lax.rem(ep + o, n)}, device_id_type=MESH)

    tokens, width = h_ref.shape
    chunks = width // COLS

    def weights(d, l):
        cols = pl.ds(pl.multiple_of(d * COLS, COLS), COLS)
        return pltpu.make_async_copy(w2_ref.at[l, :, cols], ring.at[lax.rem(d, 2), l], w_sem.at[lax.rem(d, 2), l])

    for d in range(2):
        for l in range(le):
            weights(jnp.int32(d), l).start()

    order = [(2, 0), (2, 1), (1, 0), (3, 0), (1, 1), (3, 1), (0, 1), (0, 0)]
    partner = [order.index((dx, 1 - dc)) for dx, dc in order]
    dests = [lax.rem(x + dx, chips) * 2 + lax.rem(c + dc, 2) for dx, dc in order]
    spot = pl.ds(pl.multiple_of(ep * quota, GRAN), quota)

    row = lax.broadcasted_iota(jnp.int32, (quota, le * cap), 0)
    for k in range(n):
        slots = qmap_ref[pl.ds(dests[k], 1), :]
        spread[k, pl.ds(0, quota), :] = (slots - c * quota == row).astype(F32).astype(BF16)
        spread[k, pl.ds(quota, quota), :] = (slots - (1 - c) * quota == row).astype(F32).astype(BF16)

    def swap(d, k):
        return pltpu.make_async_remote_copy(
            src_ref=away.at[lax.rem(d, 2), k], dst_ref=theirs.at[d, partner[k]], send_sem=pair_send.at[lax.rem(d, 2), k],
            recv_sem=pair_recv.at[d, partner[k]], device_id={"ep": pa}, device_id_type=MESH)

    def push(d, k):
        return pltpu.make_async_remote_copy(
            src_ref=mine.at[d, k], dst_ref=recv_buf.at[d, spot], send_sem=send_sem.at[d, k], recv_sem=recv_sem.at[d, k],
            device_id={"ep": dests[k]}, device_id_type=MESH)

    def send(d):
        for k in range(n):
            swap(d, partner[k]).wait_recv()
            if k == n - 1:
                recv_buf[d, spot, :] = mine[d, k] + theirs[d, k]
            else:
                mine[d, k] = mine[d, k] + theirs[d, k]
                push(d, k).start()

    def project(d, some):
        for l in some:
            weights(d, l).wait()
        for l in some:
            y = jnp.dot(ms_ref[l], ring[lax.rem(d, 2), l], preferred_element_type=F32)
            y_buf[:, pl.ds(l * cap, cap), :] = y.astype(BF16).reshape(n, cap, COLS)

    def chunk(d, carry):
        @pl.when(d > 1)
        def _():
            send(d - 1)

        project(d, range(le // 2, le))

        @pl.when(d + 2 < chunks)
        def _():
            for l in range(le):
                weights(d + 2, l).start()

        @pl.when(d > 1)
        def _():
            for k in range(n):
                swap(d - 2, k).wait_send()

        for k in range(n):
            both = jnp.dot(spread[k], y_buf[dests[k]], preferred_element_type=F32).astype(BF16)
            away[lax.rem(d, 2), k] = both[quota:]
            mine[d, k] = both[:quota]
        for k in range(n):
            swap(d, k).start()

        @pl.when(d == 0)
        def _():
            send(d)

        @pl.when(d + 1 < chunks)
        def _():
            project(d + 1, range(le // 2))

        return carry

    project(jnp.int32(0), range(le // 2))
    pl.semaphore_wait(bar, n - 1)
    lax.fori_loop(0, chunks, chunk, 0)
    send(jnp.int32(chunks - 1))

    def tables(r, carry):
        some = pl.ds(pl.multiple_of(r * 32, 32), 32)
        lane = lax.broadcasted_iota(jnp.int32, (32, n * quota), 1)
        for k, table in enumerate((gather0, gather1)):
            pos = (comb_ref[some, 4 + k:5 + k] * (2 * quota) + comb_ref[some, k:k + 1]).astype(jnp.int32)
            table[some, :] = (lane == pos).astype(F32).astype(BF16)
        return carry

    lax.fori_loop(0, tokens // 32, tables, 0)
    g0, g1 = comb_ref[:, 2:3], comb_ref[:, 3:4]
    alpha, beta = post_ref[0], post_ref[1]

    def finish(d, carry):
        for k in range(n - 1):
            push(d, k).wait_recv()
        cols = pl.ds(pl.multiple_of(d * COLS, COLS), COLS)
        got = recv_buf[d]
        y0 = jnp.dot(gather0[...], got, preferred_element_type=F32)
        y1 = jnp.dot(gather1[...], got, preferred_element_type=F32)
        mixed = g0 * y0 + g1 * y1
        out_ref[:, cols] = (alpha * h_ref[:, cols].astype(F32) + beta * mixed).astype(out_ref.dtype)
        for k in range(n - 1):
            push(d, k).wait_send()
        return carry

    lax.fori_loop(0, chunks, finish, 0)
    for d in range(chunks - 2, chunks):
        for k in range(n):
            swap(jnp.int32(d), k).wait_send()


def combine(n, le, cap, quota, cid, post_scale, qmap, comb, hidden, ms, w_down):
    tokens, width = hidden.shape
    ffn = ms.shape[2]
    vm = pl.BlockSpec(memory_space=pltpu.VMEM)
    sm = pl.BlockSpec(memory_space=pltpu.SMEM)
    dma = pltpu.SemaphoreType.DMA
    chunks = width // COLS
    part = pltpu.VMEM((chunks, n, quota, COLS), BF16)
    table = pltpu.VMEM((tokens, n * quota), BF16)
    return pl.pallas_call(
        functools.partial(combine_kernel, n, le, cap, quota),
        out_shape=jax.ShapeDtypeStruct((tokens, width), hidden.dtype),
        in_specs=[sm, vm, vm, vm, vm, pl.BlockSpec(memory_space=pltpu.HBM)],
        out_specs=vm,
        scratch_shapes=[pltpu.VMEM((2, le, ffn, COLS), BF16), pltpu.VMEM((n, le * cap, COLS), BF16),
                        pltpu.VMEM((n, 2 * quota, le * cap), BF16), part, part,
                        pltpu.VMEM((2, n, quota, COLS), BF16), pltpu.VMEM((chunks, n * quota, COLS), BF16), table, table,
                        dma((2, le)), dma((2, n)), dma((chunks, n)), dma((chunks, n)), dma((chunks, n))],
        compiler_params=pltpu.CompilerParams(collective_id=cid, has_side_effects=True,
                                             vmem_limit_bytes=(36 if quota <= 128 else 49) * 1024 * 1024),
        name="combine%d" % quota,
    )(post_scale, qmap, comb, hidden, ms, w_down)


def solution(mesh):
    n = mesh.shape["ep"]

    def local_step(hidden, router_w, expert_ids, w_gate, w_up, w_down, post_scale):
        tokens, width = hidden.shape
        le = w_gate.shape[0]
        cap = tokens // max(1, (n * le) // 8)
        xs, qmap, meta, comb, p1, p3 = dispatch(n, le, cap, hidden, router_w.T, expert_ids.T, w_gate, w_up)
        ms = experts(n, le, cap, meta, xs, w_gate, w_up, p1, p3)
        quotas = [q for q in (96, 128) if q < le * cap] + [le * cap]
        worst = meta[0, le]
        branch = sum((worst > 2 * q).astype(jnp.int32) for q in quotas[:-1])
        return lax.switch(branch, [functools.partial(combine, n, le, cap, q, 2 + k) for k, q in enumerate(quotas)],
                          post_scale, qmap, comb, hidden, ms, w_down)

    tok = P(("dp", "ep"))
    return jax.shard_map(local_step, mesh=mesh, in_specs=(tok, P(), tok, P("ep"), P("ep"), P("ep"), P()),
                         out_specs=tok, check_vma=False)
```

```python
import functools

import jax
import jax.numpy as jnp
from jax import lax
from jax.experimental import pallas as pl
from jax.experimental.pallas import tpu as pltpu
from jax.sharding import PartitionSpec as P

MESH = pl.DeviceIdType.MESH
PIECES = 4
GRAN = 16
BLOCK = 512
SLOTS = 6
COLS = 256
F32 = jnp.float32
BF16 = jnp.bfloat16


def dispatch_kernel(n, le, cap, h_hbm, wrt_hbm, idst_hbm, w1_ref, w3_ref, xs_ref, qmap_ref, meta_ref,
                    comb_ref, p1_ref, p3_ref, all_h, all_ids, h_ref, wrt_ref, idst_ref, send_sem, ring_sem, pair_sem,
                    in_sem, ids_send, ids_recv, w_sem):
    ep = lax.axis_index("ep")
    chips = n // 2
    x, c = ep // 2, ep % 2

    def dev(xx, cc):
        return lax.rem(xx + 2 * chips, chips) * 2 + cc

    xp, xm, pa = dev(x + 1, c), dev(x - 1, c), dev(x, 1 - c)
    inputs = [pltpu.make_async_copy(src, dst, in_sem.at[k])
              for k, (src, dst) in enumerate(((h_hbm, h_ref), (idst_hbm, idst_ref), (wrt_hbm, wrt_ref)))]
    for cp in inputs:
        cp.start()
    bar = pltpu.get_barrier_semaphore()
    for o in range(1, n):
        pl.semaphore_signal(bar, inc=1, device_id={"ep": lax.rem(ep + o, n)}, device_id_type=MESH)
    tokens, _ = h_ref.shape
    rows = tokens // PIECES
    started, loads = [], []
    inputs[0].wait()
    inputs[1].wait()
    pl.semaphore_wait(bar, n - 1)

    for o in range(1, n):
        cp = pltpu.make_async_remote_copy(
            src_ref=idst_ref, dst_ref=all_ids.at[ep], send_sem=ids_send.at[o], recv_sem=ids_recv.at[o],
            device_id={"ep": lax.rem(ep + o, n)}, device_id_type=MESH)
        cp.start()
        started.append(cp)
    own_ids = pltpu.make_async_copy(idst_ref, all_ids.at[ep], ids_recv.at[0])
    own_ids.start()

    count = [0]

    def push(src, blk, p, to, rsem):
        cp = pltpu.make_async_remote_copy(
            src_ref=src, dst_ref=all_h.at[blk, pl.ds(p * rows, rows)], send_sem=send_sem.at[count[0]], recv_sem=rsem,
            device_id={"ep": to}, device_id_type=MESH)
        count[0] += 1
        cp.start()
        started.append(cp)

    def arrive(blk, p, sem):
        ref = all_h.at[blk, pl.ds(p * rows, rows)]
        pltpu.make_async_remote_copy(src_ref=ref, dst_ref=ref, send_sem=send_sem.at[0], recv_sem=sem,
                                     device_id={"ep": pa}, device_id_type=MESH).wait_recv()

    last = PIECES - 1
    for s in range(PIECES):
        push(h_ref.at[pl.ds(s * rows, rows)], ep, s, xp, ring_sem.at[0, s])
        push(h_ref.at[pl.ds((last - s) * rows, rows)], ep, last - s, xm, ring_sem.at[1, last - s])
    for s in range(PIECES):
        push(h_ref.at[pl.ds(s * rows, rows)], ep, s, pa, pair_sem.at[0, s])

    steps = w1_ref.shape[2] // BLOCK
    for s in range(SLOTS):
        cols = pl.ds(s % steps * BLOCK, BLOCK)
        for k, (src, dst) in enumerate(((w1_ref, p1_ref), (w3_ref, p3_ref))):
            cp = pltpu.make_async_copy(src.at[s // steps, :, cols], dst.at[s], w_sem.at[s, k])
            cp.start()
            loads.append(cp)

    inputs[2].wait()
    own_ids.wait()
    for o in range(1, n):
        ref = all_ids.at[lax.rem(ep + n - o, n)]
        pltpu.make_async_remote_copy(src_ref=ref, dst_ref=ref, send_sem=ids_send.at[o], recv_sem=ids_recv.at[o],
                                     device_id={"ep": pa}, device_id_type=MESH).wait_recv()
    ids0 = all_ids[:, 0, :]
    ids1 = all_ids[:, 1, :]
    experts = n * le
    upper = (lax.broadcasted_iota(jnp.int32, (tokens, tokens), 0)
             < lax.broadcasted_iota(jnp.int32, (tokens, tokens), 1)).astype(F32).astype(BF16)

    def hits(lo, hi):
        return (jnp.where((ids0 >= lo) & (ids0 < hi), 1.0, 0.0) + jnp.where((ids1 >= lo) & (ids1 < hi), 1.0, 0.0))

    lane = lax.broadcasted_iota(jnp.int32, (n, le * cap), 1)
    lane_m = lax.broadcasted_iota(jnp.int32, meta_ref.shape, 1)
    qmap = jnp.full((n, le * cap), -1.0, F32)
    meta = jnp.zeros(meta_ref.shape, F32)
    offset = jnp.where(c > 0, 1.0, 0.0) * jnp.sum(hits(x * 2 * le, x * 2 * le + le), axis=1, keepdims=True)
    slots = []
    for l in range(le):
        e = ep * le + l
        mask = jnp.where((ids0 == e) | (ids1 == e), 1.0, 0.0)
        rank = jnp.dot(mask.astype(BF16), upper, preferred_element_type=F32)
        slots.append(jnp.where(mask > 0.5, rank, -1.0).astype(jnp.int32))
        cnt = jnp.sum(mask, axis=1, keepdims=True)
        inside = lane - l * cap
        insidef = inside.astype(F32)
        qmap = jnp.where((inside >= 0) & (inside < cap) & (insidef < cnt), offset + insidef, qmap)
        meta = jnp.where(lane_m == l, cnt, meta)
        offset = offset + cnt
    qmap_ref[...] = qmap.astype(jnp.int32)
    worst = jnp.zeros((n, 1), F32)
    for j in range(chips):
        worst = jnp.maximum(worst, jnp.sum(hits(j * 2 * le, (j + 1) * 2 * le), axis=1, keepdims=True))
    worst = jnp.max(worst, axis=0, keepdims=True)
    meta_ref[...] = jnp.where(lane_m == le, worst, meta).astype(jnp.int32)

    own0, own1 = idst_ref[0:1, :], idst_ref[1:2, :]
    sub = lax.broadcasted_iota(jnp.int32, (experts, tokens), 0)
    logits = lax.dot_general(wrt_ref[...], h_ref[...].astype(F32), (((1,), (1,)), ((), ())),
                             precision=lax.Precision.HIGHEST, preferred_element_type=F32)
    ex = jnp.exp(logits - jnp.max(logits, axis=0, keepdims=True))
    prob = ex / jnp.sum(ex, axis=0, keepdims=True)
    pick0, pick1 = sub == own0, sub == own1
    p0 = jnp.sum(jnp.where(pick0, prob, 0.0), axis=0, keepdims=True)
    p1 = jnp.sum(jnp.where(pick1, prob, 0.0), axis=0, keepdims=True)
    hot = jnp.where(pick0 | pick1, 1.0, 0.0)
    rank = jnp.dot(hot.astype(BF16), upper, preferred_element_type=F32)
    ei = lax.broadcasted_iota(jnp.int32, (experts, experts), 0)
    ej = lax.broadcasted_iota(jnp.int32, (experts, experts), 1)
    before = ((ei // (2 * le) == ej // (2 * le)) & (ej < ei)).astype(F32).astype(BF16)
    total = jnp.broadcast_to(jnp.sum(hot, axis=1, keepdims=True), (experts, 128)).astype(BF16)
    base = jnp.dot(before, total, preferred_element_type=F32)[:, 0:1]
    where = rank + base
    pos0 = jnp.sum(jnp.where(pick0, where, 0.0), axis=0, keepdims=True)
    pos1 = jnp.sum(jnp.where(pick1, where, 0.0), axis=0, keepdims=True)
    chip0, chip1 = (own0 // (2 * le)).astype(F32), (own1 // (2 * le)).astype(F32)
    row = lax.broadcasted_iota(jnp.int32, (128, tokens), 0)
    packed = jnp.zeros((128, tokens), F32)
    for k, v in enumerate((pos0, pos1, p0 / (p0 + p1), p1 / (p0 + p1), chip0, chip1)):
        packed = jnp.where(row == k, v, packed)
    comb_ref[...] = packed.T

    slot_row = lax.broadcasted_iota(jnp.int32, (cap, tokens), 0)

    def place(i, src):
        one_hot = []
        for l in range(le):
            one = slots[l]
            pick = jnp.sum(jnp.where(lax.broadcasted_iota(jnp.int32, one.shape, 0) == i, one, 0), axis=0, keepdims=True)
            one_hot.append((pick == slot_row).astype(F32).astype(BF16))
        one_hot = jnp.concatenate(one_hot, axis=0)
        half = src.shape[1] // 2
        for q in range(2):
            cols = pl.ds(q * half, half)
            got = jnp.dot(one_hot, src[:, cols], preferred_element_type=F32).astype(BF16)
            for l in range(le):
                xs_ref[l, pl.ds(pl.multiple_of(i * cap, cap), cap), cols] = got[l * cap:(l + 1) * cap]

    place(ep, h_ref)

    bm, bp, b2 = dev(x - 1, c), dev(x + 1, c), dev(x + 2, c)
    for s in range(PIECES):
        q = last - s
        arrive(bm, s, ring_sem.at[0, s])
        ref = all_h.at[bm, pl.ds(s * rows, rows)]
        if s < PIECES // 2:
            push(ref, bm, s, xp, ring_sem.at[2, s])
        push(ref, bm, s, pa, pair_sem.at[1, s])
        arrive(bp, q, ring_sem.at[1, q])
        ref = all_h.at[bp, pl.ds(q * rows, rows)]
        if s < PIECES // 2:
            push(ref, bp, q, xm, ring_sem.at[2, q])
        push(ref, bp, q, pa, pair_sem.at[2, q])
    def landed(i, xx):
        for s in range(PIECES):
            arrive(dev(xx, 1 - c), s, pair_sem.at[i, s])

    landed(0, x)
    place(pa, all_h.at[pa])
    place(bm, all_h.at[bm])
    place(bp, all_h.at[bp])
    for k, xx in enumerate((x - 1, x + 1)):
        landed(1 + k, xx)
        place(dev(xx, 1 - c), all_h.at[dev(xx, 1 - c)])
    for r in range(PIECES // 2):
        for q in (r, last - r):
            arrive(b2, q, ring_sem.at[2, q])
            push(all_h.at[b2, pl.ds(q * rows, rows)], b2, q, pa, pair_sem.at[3, q])
    place(b2, all_h.at[b2])
    landed(3, x + 2)
    place(dev(x + 2, 1 - c), all_h.at[dev(x + 2, 1 - c)])
    for cp in started:
        cp.wait_send()
    for cp in loads:
        cp.wait()


def dispatch(n, le, cap, hidden, router_wt, ids_t, w_gate, w_up):
    tokens, width = hidden.shape
    vm = pl.BlockSpec(memory_space=pltpu.VMEM)
    hbm = pl.BlockSpec(memory_space=pltpu.HBM)
    dma = pltpu.SemaphoreType.DMA
    ring = jax.ShapeDtypeStruct((SLOTS, width, BLOCK), BF16)
    return pl.pallas_call(
        functools.partial(dispatch_kernel, n, le, cap),
        out_shape=(jax.ShapeDtypeStruct((le, n * cap, width), hidden.dtype),
                   jax.ShapeDtypeStruct((n, le * cap), jnp.int32),
                   jax.ShapeDtypeStruct((n, 128), jnp.int32),
                   jax.ShapeDtypeStruct((tokens, 128), F32), ring, ring),
        in_specs=[hbm, hbm, hbm, hbm, hbm],
        out_specs=(vm, vm, vm, vm, vm, vm),
        scratch_shapes=[pltpu.VMEM((n, tokens, width), BF16), pltpu.VMEM((n, 2, tokens), jnp.int32),
                        pltpu.VMEM((tokens, width), BF16), pltpu.VMEM(router_wt.shape, F32),
                        pltpu.VMEM(ids_t.shape, jnp.int32), dma((PIECES * 7,)), dma((3, PIECES)), dma((4, PIECES)),
                        dma((3,)), dma((n,)), dma((n,)), dma((SLOTS, 2))],
        compiler_params=pltpu.CompilerParams(collective_id=1, has_side_effects=True,
                                             vmem_limit_bytes=16 * 1024 * 1024),
        name="dispatch",
    )(*[pltpu.with_memory_space_constraint(a, pltpu.HBM) for a in (hidden, router_wt, ids_t, w_gate, w_up)])


def experts_kernel(n, le, cap, meta_ref, xs_ref, w1_ref, w3_ref, _p1, _p3, w2_ref, ms_ref, b1, b3, y0_ref, x_buf, m_buf,
                   w2_buf, w_sem, w2_sem):
    width, ffn = w1_ref.shape[1:]
    steps = ffn // BLOCK
    total = le * steps

    def weights(s, act):
        l, f, k = s // steps, s % steps, s % SLOTS
        cols = pl.ds(pl.multiple_of(f * BLOCK, BLOCK), BLOCK)
        act(pltpu.make_async_copy(w1_ref.at[l, :, cols], b1.at[k], w_sem.at[k, 0]))
        act(pltpu.make_async_copy(w3_ref.at[l, :, cols], b3.at[k], w_sem.at[k, 1]))

    def down(l):
        return pltpu.make_async_copy(w2_ref.at[l, :, pl.ds(0, COLS)], w2_buf.at[l], w2_sem.at[l])

    for l in range(le):
        down(l).start()

    def run(l, part):
        rows = n * part
        if part < cap:
            for i in range(n):
                x_buf[pl.ds(i * part, part), :] = xs_ref[l, pl.ds(i * cap, part), :]
                ms_ref[l, pl.ds(i * cap + part, cap - part), :] = jnp.zeros((cap - part, ffn), BF16)

        def step(f, carry):
            s = l * steps + f
            k = s % SLOTS

            @pl.when((s > 0) & (s + SLOTS - 1 < total))
            def _():
                weights(s + SLOTS - 1, lambda cp: cp.start())

            @pl.when(s >= SLOTS)
            def _():
                weights(s, lambda cp: cp.wait())

            xt = x_buf[pl.ds(0, rows), :] if part < cap else xs_ref[l]
            for j in range(BLOCK // 256):
                cols = pl.ds(j * 256, 256)
                a = jnp.dot(xt, b1[k, :, cols], preferred_element_type=F32)
                b = jnp.dot(xt, b3[k, :, cols], preferred_element_type=F32)
                mid = (a * jax.nn.sigmoid(a) * b).astype(BF16)
                out = pl.ds(pl.multiple_of(f * BLOCK + j * 256, 256), 256)
                if part < cap:
                    m_buf[pl.ds(0, rows), out] = mid
                    for i in range(n):
                        ms_ref[l, pl.ds(i * cap, part), out] = mid[i * part:(i + 1) * part]
                else:
                    ms_ref[l, :, out] = mid
            return carry

        lax.fori_loop(0, steps, step, 0)

        down(l).wait()
        mt = m_buf[pl.ds(0, rows), :] if part < cap else ms_ref[l]
        y = jnp.dot(mt, w2_buf[l], preferred_element_type=F32).astype(BF16)
        at = pl.multiple_of(l * cap, cap)
        for i in range(n):
            y0_ref[i, pl.ds(at, part), :] = y[i * part:(i + 1) * part]
            if part < cap:
                y0_ref[i, pl.ds(at + part, cap - part), :] = jnp.zeros((cap - part, COLS), BF16)

    def expert(l, carry):
        most = meta_ref[0, l]
        for i in range(1, n):
            most = jnp.maximum(most, meta_ref[i, l])
        parts = (GRAN, 2 * GRAN, cap)
        for k, part in enumerate(parts):
            low = parts[k - 1] if k else -1
            high = part if part < cap else n * cap

            @pl.when((most > low) & (most <= high))
            def _():
                run(l, part)

        return carry

    lax.fori_loop(0, le, expert, 0)


def experts(n, le, cap, meta, xs, w_gate, w_up, p1, p3, w_down):
    width, ffn = w_gate.shape[1:]
    full = n * cap
    hbm = pl.BlockSpec(memory_space=pltpu.HBM)
    vm = pl.BlockSpec(memory_space=pltpu.VMEM)
    dma = pltpu.SemaphoreType.DMA
    return pl.pallas_call(
        functools.partial(experts_kernel, n, le, cap),
        out_shape=(jax.ShapeDtypeStruct((le, full, ffn), BF16), jax.ShapeDtypeStruct(p1.shape, BF16),
                   jax.ShapeDtypeStruct(p3.shape, BF16), jax.ShapeDtypeStruct((n, le * cap, COLS), BF16)),
        in_specs=[pl.BlockSpec(memory_space=pltpu.SMEM), vm, hbm, hbm, vm, vm, hbm],
        out_specs=(vm, vm, vm, vm),
        input_output_aliases={4: 1, 5: 2},
        scratch_shapes=[pltpu.VMEM((n * 2 * GRAN, width), BF16), pltpu.VMEM((n * 2 * GRAN, ffn), BF16),
                        pltpu.VMEM((le, ffn, COLS), BF16), dma((SLOTS, 2)), dma((le,))],
        compiler_params=pltpu.CompilerParams(vmem_limit_bytes=13 * 1024 * 1024),
        name="experts",
    )(meta, xs, w_gate, w_up, p1, p3, w_down)


def combine_kernel(n, le, cap, quota, post_ref, qmap_ref, comb_ref, h_ref, ms_ref, y0_ref, w2_ref, out_ref,
                   ring, y_buf, spread, mine, theirs, away, recv_buf, gather0, gather1, w_sem, pair_send, pair_recv,
                   send_sem, recv_sem):
    ep = lax.axis_index("ep")
    chips = n // 2
    x, c = ep // 2, ep % 2
    pa = x * 2 + 1 - c
    bar = pltpu.get_barrier_semaphore()
    for o in range(1, n):
        pl.semaphore_signal(bar, inc=1, device_id={"ep": lax.rem(ep + o, n)}, device_id_type=MESH)

    tokens, width = h_ref.shape
    chunks = width // COLS

    def weights(d, l):
        cols = pl.ds(pl.multiple_of(d * COLS, COLS), COLS)
        return pltpu.make_async_copy(w2_ref.at[l, :, cols], ring.at[lax.rem(d, 2), l], w_sem.at[lax.rem(d, 2), l])

    for d in range(1, 3):
        for l in range(le):
            weights(jnp.int32(d), l).start()

    order = [(2, 0), (2, 1), (1, 0), (3, 0), (1, 1), (3, 1), (0, 1), (0, 0)]
    partner = [order.index((dx, 1 - dc)) for dx, dc in order]
    dests = [lax.rem(x + dx, chips) * 2 + lax.rem(c + dc, 2) for dx, dc in order]
    spot = pl.ds(pl.multiple_of(ep * quota, GRAN), quota)

    row = lax.broadcasted_iota(jnp.int32, (quota, le * cap), 0)
    for k in range(n):
        slots = qmap_ref[pl.ds(dests[k], 1), :]
        spread[k, pl.ds(0, quota), :] = (slots - c * quota == row).astype(F32).astype(BF16)
        spread[k, pl.ds(quota, quota), :] = (slots - (1 - c) * quota == row).astype(F32).astype(BF16)

    def swap(d, k):
        return pltpu.make_async_remote_copy(
            src_ref=away.at[lax.rem(d, 2), k], dst_ref=theirs.at[d, partner[k]], send_sem=pair_send.at[lax.rem(d, 2), k],
            recv_sem=pair_recv.at[d, partner[k]], device_id={"ep": pa}, device_id_type=MESH)

    def push(d, k):
        return pltpu.make_async_remote_copy(
            src_ref=mine.at[d, k], dst_ref=recv_buf.at[d, spot], send_sem=send_sem.at[d, k], recv_sem=recv_sem.at[d, k],
            device_id={"ep": dests[k]}, device_id_type=MESH)

    def send(d):
        for k in range(n):
            swap(d, partner[k]).wait_recv()
            if k == n - 1:
                recv_buf[d, spot, :] = mine[d, k] + theirs[d, k]
            else:
                mine[d, k] = mine[d, k] + theirs[d, k]
                push(d, k).start()

    def project(d, some):
        for l in some:
            weights(d, l).wait()
        for l in some:
            y = jnp.dot(ms_ref[l], ring[lax.rem(d, 2), l], preferred_element_type=F32)
            y_buf[:, pl.ds(l * cap, cap), :] = y.astype(BF16).reshape(n, cap, COLS)

    def chunk(d, carry):
        @pl.when(d > 1)
        def _():
            send(d - 1)

        @pl.when(d > 0)
        def _():
            project(d, range(le // 2, le))

        @pl.when((d > 0) & (d + 2 < chunks))
        def _():
            for l in range(le):
                weights(d + 2, l).start()

        @pl.when(d > 1)
        def _():
            for k in range(n):
                swap(d - 2, k).wait_send()

        for k in range(n):
            both = jnp.dot(spread[k], y_buf[dests[k]], preferred_element_type=F32).astype(BF16)
            away[lax.rem(d, 2), k] = both[quota:]
            mine[d, k] = both[:quota]
        for k in range(n):
            swap(d, k).start()

        @pl.when(d == 0)
        def _():
            send(d)

        @pl.when(d + 1 < chunks)
        def _():
            project(d + 1, range(le // 2))

        return carry

    y_buf[...] = y0_ref[...]
    pl.semaphore_wait(bar, n - 1)
    lax.fori_loop(0, chunks, chunk, 0)
    send(jnp.int32(chunks - 1))

    def tables(r, carry):
        some = pl.ds(pl.multiple_of(r * 32, 32), 32)
        lane = lax.broadcasted_iota(jnp.int32, (32, n * quota), 1)
        for k, table in enumerate((gather0, gather1)):
            pos = (comb_ref[some, 4 + k:5 + k] * (2 * quota) + comb_ref[some, k:k + 1]).astype(jnp.int32)
            table[some, :] = (lane == pos).astype(F32).astype(BF16)
        return carry

    lax.fori_loop(0, tokens // 32, tables, 0)
    g0, g1 = comb_ref[:, 2:3], comb_ref[:, 3:4]
    alpha, beta = post_ref[0], post_ref[1]

    def finish(d, carry):
        for k in range(n - 1):
            push(d, k).wait_recv()
        cols = pl.ds(pl.multiple_of(d * COLS, COLS), COLS)
        got = recv_buf[d]
        y0 = jnp.dot(gather0[...], got, preferred_element_type=F32)
        y1 = jnp.dot(gather1[...], got, preferred_element_type=F32)
        mixed = g0 * y0 + g1 * y1
        out_ref[:, cols] = (alpha * h_ref[:, cols].astype(F32) + beta * mixed).astype(out_ref.dtype)
        for k in range(n - 1):
            push(d, k).wait_send()
        return carry

    lax.fori_loop(0, chunks, finish, 0)
    for d in range(chunks - 2, chunks):
        for k in range(n):
            swap(jnp.int32(d), k).wait_send()


def combine(n, le, cap, quota, cid, post_scale, qmap, comb, hidden, ms, y0, w_down):
    tokens, width = hidden.shape
    ffn = ms.shape[2]
    vm = pl.BlockSpec(memory_space=pltpu.VMEM)
    sm = pl.BlockSpec(memory_space=pltpu.SMEM)
    dma = pltpu.SemaphoreType.DMA
    chunks = width // COLS
    part = pltpu.VMEM((chunks, n, quota, COLS), BF16)
    table = pltpu.VMEM((tokens, n * quota), BF16)
    return pl.pallas_call(
        functools.partial(combine_kernel, n, le, cap, quota),
        out_shape=jax.ShapeDtypeStruct((tokens, width), hidden.dtype),
        in_specs=[sm, vm, vm, vm, vm, vm, pl.BlockSpec(memory_space=pltpu.HBM)],
        out_specs=vm,
        scratch_shapes=[pltpu.VMEM((2, le, ffn, COLS), BF16), pltpu.VMEM((n, le * cap, COLS), BF16),
                        pltpu.VMEM((n, 2 * quota, le * cap), BF16), part, part,
                        pltpu.VMEM((2, n, quota, COLS), BF16), pltpu.VMEM((chunks, n * quota, COLS), BF16), table, table,
                        dma((2, le)), dma((2, n)), dma((chunks, n)), dma((chunks, n)), dma((chunks, n))],
        compiler_params=pltpu.CompilerParams(collective_id=cid, has_side_effects=True,
                                             vmem_limit_bytes=(34 if quota <= 128 else 47) * 1024 * 1024),
        name="combine%d" % quota,
    )(post_scale, qmap, comb, hidden, ms, y0, w_down)


def solution(mesh):
    n = mesh.shape["ep"]

    def local_step(hidden, router_w, expert_ids, w_gate, w_up, w_down, post_scale):
        tokens, width = hidden.shape
        le = w_gate.shape[0]
        cap = tokens // max(1, (n * le) // 8)
        xs, qmap, meta, comb, p1, p3 = dispatch(n, le, cap, hidden, router_w.T, expert_ids.T, w_gate, w_up)
        ms, _, _, y0 = experts(n, le, cap, meta, xs, w_gate, w_up, p1, p3, w_down)
        quotas = [q for q in (96, 128) if q < le * cap] + [le * cap]
        worst = meta[0, le]
        branch = sum((worst > 2 * q).astype(jnp.int32) for q in quotas[:-1])
        return lax.switch(branch, [functools.partial(combine, n, le, cap, q, 2 + k) for k, q in enumerate(quotas)],
                          post_scale, qmap, comb, hidden, ms, y0, w_down)

    tok = P(("dp", "ep"))
    return jax.shard_map(local_step, mesh=mesh, in_specs=(tok, P(), tok, P("ep"), P("ep"), P("ep"), P()),
                         out_specs=tok, check_vma=False)
```
